32 devices in a mesh: seq: 8 (over y, x, core), mp: 4 (over z).
Axes of the slice: x: 2, y: 2, z: 4, core: 2. Of those that a mesh axis runs over, the one named last changes fastest.
Arguments:
- inputs: bfloat16 [8192, 4096], P('seq', 'mp'), may hold values from -6 to 6
- conv_weight: bfloat16 [4, 4096], P(None, 'mp'), may hold values from -3 to 3
- conv_bias: bfloat16 [4096], P('mp'), may hold values from -3 to 3
- doc_start: int32 [8192], P('seq'), may hold values from 0 to 8191, as said below
- counts: int32 [8], P('seq'), may hold values from 341 to 1024
Outputs:
- gram: float32 [4096, 4096], P('seq', 'mp')
The draws below stay inside these ranges and needn't reach their ends.
Inputs may be any that keep to these rules, and one draw needn't show every extreme that they name: doc_start is never above the token's own position, and for t > 0 either doc_start[t] == t or doc_start[t] == doc_start[t - 1]; doc_start[0] is 0.
All inputs are finite; a program needn't handle non-finite values.
Results may differ from the reference program's by a relative error of at most 0.0003.
Values may be sent and summed in bfloat16 or wider, within the bound.
A program may use at most 64 MiB of HBM per device.

```python
import jax
import jax.numpy as jnp
from jax import lax

C = 4096
KERNEL = 4
TOK_DEV = 1024
TOKENS = 8192
SHARDS = 8


def draw_doc_start(key, part):
    flags = jax.random.randint(key, (TOKENS,), 0, max(TOK_DEV // 4, 2)) == 0
    flags = flags.at[0].set(True).at[TOKENS - 1].set(True)
    position = jnp.arange(TOKENS, dtype=jnp.int32)
    starts = jnp.where(flags, position, 0)
    return lax.cummax(starts, axis=0).astype(jnp.int32)


def draw_counts(key, part):
    shard_ids = jnp.arange(SHARDS, dtype=jnp.int32)
    spread = TOK_DEV - TOK_DEV // 3 - TOK_DEV // 8
    base = TOK_DEV // 3 + shard_ids * spread // (SHARDS - 1)
    jitter = jax.random.randint(key, (SHARDS,), 0, TOK_DEV // 8 + 1)
    values = jnp.minimum(base + jitter, TOK_DEV)
    return values.at[SHARDS - 1].set(TOK_DEV).astype(jnp.int32)


def block_scale(key, dims, pieces, low, top_value):
    loudness, own = 1.0, jax.random.fold_in(key, 6)
    for axis_at, blocks in pieces:
        draws = jnp.exp(jax.random.uniform(jax.random.fold_in(own, axis_at), (blocks,), jnp.float32, low / len(pieces), top_value / len(pieces)))
        loudness = loudness * jnp.repeat(draws, dims[axis_at] // blocks).reshape([-1 if axis == axis_at else 1 for axis in range(len(dims))])
    return loudness


def gaussian(stream_key, extent, scale, most, split=(), kind=jnp.bfloat16):
    entries = jax.random.normal(stream_key, extent, jnp.float32) * scale
    if len(split) > 0:
        entries = block_scale(stream_key, extent, split, -0.22, 0.18) * entries
    return jnp.clip(entries, min=-most, max=most).astype(kind)


def setup_inputs(seed: int = 0) -> dict:
    seeds = jax.random.split(jax.random.key(seed), 6)
    return {
        "inputs": gaussian(seeds[0], (TOKENS, C), 1.0, 6.0, ((0, 8), (1, 4))),
        "conv_weight": gaussian(seeds[1], (KERNEL, C), KERNEL ** -0.5, 3.0, ((1, 4),)),
        "conv_bias": gaussian(seeds[2], (C,), 0.5, 3.0, ((0, 4),)),
        "doc_start": draw_doc_start(jax.random.fold_in(seeds[5], 71), 0),
        "counts": draw_counts(jax.random.fold_in(seeds[5], 71), 0),
    }


def causal_conv(extended, weights, bias, position, doc_start, length):
    kernel_len = weights.shape[0]
    summed = jnp.zeros((length, weights.shape[1]), jnp.float32) + bias.astype(jnp.float32)
    for lag in range(kernel_len):
        window = extended[kernel_len - 1 - lag: kernel_len - 1 - lag + length].astype(jnp.float32)
        usable = (position - lag) >= doc_start
        summed = summed + jnp.where(usable[:, None], weights[lag].astype(jnp.float32) * window, 0.0)
    return jax.nn.silu(summed).astype(jnp.bfloat16)


def reference(inputs, conv_weight, conv_bias, doc_start, counts):
    position = jnp.arange(TOKENS, dtype=jnp.int32)
    padding = jnp.zeros((KERNEL - 1, C), jnp.bfloat16)
    extended = jnp.concatenate([padding, inputs], axis=0)
    feats = causal_conv(extended, conv_weight, conv_bias, position, doc_start, TOKENS)
    counted = (position % TOK_DEV) < jnp.repeat(counts, TOK_DEV)
    kept = jnp.where(counted[:, None], feats, jnp.zeros_like(feats))

    def add_block(carry, pair):
        left, right = pair
        return carry + lax.dot_general(left, right, (((0,), (0,)), ((), ())), preferred_element_type=jnp.float32), None

    summed, _ = lax.scan(add_block, jnp.zeros((C, C), jnp.float32),
                         (feats.reshape(SHARDS, TOK_DEV, C), kept.reshape(SHARDS, TOK_DEV, C)))
    token_total = jnp.sum(counts.astype(jnp.float32))
    return summed / token_total
```

```python
import functools

import jax
import jax.numpy as jnp
from jax import lax
from jax.experimental import pallas as pl
from jax.experimental.pallas import tpu as pltpu
from jax.sharding import PartitionSpec as P

MESH = pl.DeviceIdType.MESH
LANES = 128
HALO = 16


def when(cond):
    return pl.when(cond)


TINY = 1e-30
STEPS = 32767.0


class Group:
    def __init__(self, *copies):
        self.copies = copies

    def start(self):
        for copy in self.copies:
            copy.start()

    def wait_send(self):
        for copy in self.copies:
            copy.wait_send()

    def wait_recv(self):
        for copy in self.copies:
            copy.wait_recv()


def gram_kernel(peers, depth, taps, near, relayed, x_hbm, taps_ref, bias_ref, doc_ref, counts_ref, o_ref, ext, feats, got, part,
                from_x, from_y, sum_y, sum_x, rim, rpart, rfrom_x, rfrom_y, rsum_y, rsum_x, ready, readyu, landed, landedu, totals,
                lag_ref, cnt_ref, bias_rows, code, unit, from_xu, from_yu, sum_yu, sum_xu, rcode, runit, rfrom_xu, rfrom_yu, rsum_yu, rsum_xu,
                load_sem, halo_sem, cnt_send, cnt_recv, pair_send, pair_recv,
                up_send, down_send, fwd_send, got_recv,
                a1_send, a1_recv, b1_send, b1_recv, a2_send, a2_recv, b2_send, b2_recv,
                share_send, share_recv, ra1_send, ra1_recv, rb1_send, rb1_recv,
                ra2_send, ra2_recv, rb2_send, rb2_recv, land_send, land_recv):
    s, z = lax.axis_index("seq"), lax.axis_index("mp")
    core, x, y = lax.rem(s, 2), lax.rem(s // 2, 2), s // 4
    sib, over_x, over_y = s + 1 - 2 * core, s + 2 - 4 * x, s + 4 - 8 * y
    quad = s // 2
    rows, width = x_hbm.shape
    half = width // 2
    pieces = half // LANES
    on_rim = jnp.logical_or(z == 0, z == depth - 1)
    inside = jnp.logical_not(on_rim)
    orient = jnp.where(z < depth // 2, 1, -1)
    outer = jnp.where(z < depth // 2, 0, depth - 1)

    def remote(src, dst, send, recv, to):
        return pltpu.make_async_remote_copy(src_ref=src, dst_ref=dst, send_sem=send, recv_sem=recv,
                                            device_id=to, device_id_type=MESH)

    def both(*conds):
        return functools.reduce(jnp.logical_and, conds)

    def either(*conds):
        return functools.reduce(jnp.logical_or, conds)

    load = pltpu.make_async_copy(x_hbm, ext.at[pl.ds(HALO, rows)], load_sem)
    load.start()

    barrier = pltpu.get_barrier_semaphore()
    for step in range(1, peers):
        pl.semaphore_signal(barrier, inc=1, device_id=(lax.rem(s + step, peers), z), device_id_type=MESH)

    @when(z > 0)
    def _():
        pl.semaphore_signal(barrier, inc=1, device_id=(s, z - 1), device_id_type=MESH)

    @when(z < depth - 1)
    def _():
        pl.semaphore_signal(barrier, inc=1, device_id=(s, z + 1), device_id_type=MESH)

    bias_rows[...] = bias_ref[...].astype(jnp.float32)
    cnt_ref[...] = jnp.broadcast_to(counts_ref[0], cnt_ref.shape)
    block = LANES

    def mark_block(r, _):
        first = pl.multiple_of(r * block, block)
        within = first + lax.broadcasted_iota(jnp.int32, (block, LANES), 0)
        start = jnp.transpose(jnp.broadcast_to(doc_ref[pl.ds(r, 1), :], (block, LANES)))
        reach = jnp.minimum(s * rows + within - start, taps - 1)
        lag_ref[pl.ds(first, block), :] = reach + jnp.where(within < counts_ref[0], taps, 0)
        return 0

    lax.fori_loop(0, rows // block, mark_block, 0)

    load.wait()
    pl.semaphore_wait(barrier, peers - 1 + jnp.where(z > 0, 1, 0) + jnp.where(z < depth - 1, 1, 0))

    halo = remote(ext.at[pl.ds(rows, HALO)], ext.at[pl.ds(0, HALO)], halo_sem.at[0], halo_sem.at[1],
                  (lax.rem(s + 1, peers), z))

    @when(s < peers - 1)
    def _():
        halo.start()

    def cnt_copy(step, slot):
        return remote(cnt_ref, totals.at[slot], cnt_send.at[step], cnt_recv.at[slot],
                      (lax.rem(s + step, peers), z))

    for step in range(1, peers):
        cnt_copy(step, s).start()

    own_rows = pl.multiple_of(core * rows, rows)

    def conv(column, low, high):
        at = pl.ds(pl.multiple_of(column, LANES), LANES)
        taps_here = taps_ref[:, at].astype(jnp.float32)
        bias_here = bias_rows[pl.ds(column // LANES, 1), :]

        def body(r, _):
            first = pl.multiple_of(r * block, block)
            seen = ext[pl.ds(first, block + HALO), at].astype(jnp.float32)
            mark = lag_ref[pl.ds(first, block), :]
            lags = jnp.bitwise_and(mark, taps - 1)
            total = jnp.broadcast_to(bias_here, (block, LANES))
            for lag_ in range(taps):
                window = (pltpu.roll(seen, lag_, 0) if lag_ else seen)[HALO:]
                term = jnp.broadcast_to(taps_here[lag_ : lag_ + 1], (block, LANES)) * window
                total = total + jnp.where(lags >= lag_, term, 0.0)
            value = total / (1.0 + jnp.exp(-total))
            value = jnp.where(mark >= taps, value, 0.0)
            feats[pl.ds(pl.multiple_of(own_rows + first, block), block), at] = value.astype(feats.dtype)
            return 0

        lax.fori_loop(low, high, body, 0)

    def pair_copy(piece, row0):
        spot = feats.at[pl.ds(row0, rows), pl.ds(pl.multiple_of(piece * LANES, LANES), LANES)]
        return remote(spot, spot, pair_send.at[piece], pair_recv.at[piece], (sib, z))

    def own_columns(k):
        return pl.ds(pl.multiple_of(core * half + k * LANES, LANES), LANES)

    def tokens(j):
        return pl.ds(pl.multiple_of(j * rows, rows), rows)

    def up_copy(k, j):
        return remote(feats.at[tokens(j), own_columns(k)], got.at[z, k, tokens(j)], up_send.at[k, j],
                      got_recv.at[z, k, j], (s, lax.rem(z + 1, depth)))

    def down_copy(k, j):
        return remote(feats.at[tokens(j), own_columns(k)], got.at[z, k, tokens(j)], down_send.at[k, j],
                      got_recv.at[z, k, j], (s, lax.rem(z + depth - 1, depth)))

    def goes_up(k):
        return either(z < depth - 2, both(z == depth - 2, k >= near))

    def goes_down(k):
        return either(z > 1, both(z == 1, k >= near))

    blocks = rows // block
    for side in (1 - core, core):
        conv(side * half, 1, blocks)

    @when(s == 0)
    def _():
        ext[0:HALO, :] = jnp.zeros((HALO, width), ext.dtype)

    @when(s > 0)
    def _():
        halo.wait_recv()

    def spread(k, _):
        def make(side):
            piece = side * pieces + k
            conv(piece * LANES, 0, jnp.where(k == 0, 1, blocks))
            pair_copy(piece, own_rows).start()


        def send(j):
            @when(goes_up(k))
            def _():
                up_copy(k, j).start()

            @when(goes_down(k))
            def _():
                down_copy(k, j).start()

        make(1 - core)
        make(core)
        send(core)
        pair_copy(core * pieces + k, own_rows).wait_recv()
        send(1 - core)
        return 0

    lax.fori_loop(0, pieces, spread, 0)

    def settle(k, _):
        pair_copy((1 - core) * pieces + k, own_rows).wait_recv()
        got[z, k] = feats[:, own_columns(k)]
        return 0

    lax.fori_loop(0, pieces, settle, 0)

    steps = pieces + 2 * pieces * (depth - 1)

    def quota(span):
        return jnp.where(span == depth - 1, relayed, near)

    def place(i):
        later = i - pieces
        own = i < pieces
        later = jnp.where(own, 0, later)
        away = jnp.where(own, 0, later // (2 * pieces) + 1)
        k = jnp.where(own, i, lax.rem(later, 2 * pieces) // 2)
        second = both(jnp.logical_not(own), lax.rem(later, 2) == 1)
        sign = jnp.where(second, -orient, orient)
        block_at = z + sign * away
        within = both(block_at >= 0, block_at < depth)
        block_in = jnp.where(within, block_at, 0)
        valid = both(within, either(own, inside, k >= quota(away)))
        relay = both(inside, away == 2, second)
        return away, k, sign, block_in, valid, second, relay

    def onward(away, k, sign, valid):
        beyond = z - sign
        deep = both(beyond > 0, beyond < depth - 1)
        edge = either(beyond == 0, beyond == depth - 1)
        return both(valid, away > 0, either(deep, both(edge, k >= quota(away + 1))))

    def apart(block_at):
        return lax.rem(block_at, 2) != x, block_at // 2 != y

    def fwd_copy(block_at, k, j, sign):
        to = lax.rem(z - sign + depth, depth)
        return remote(got.at[block_at, k, tokens(j)], got.at[block_at, k, tokens(j)], fwd_send.at[block_at, k, j],
                      got_recv.at[block_at, k, j], (s, to))

    def coded(src, srcu, dst, dstu, send, recv, to):
        return Group(remote(src, dst, send.at[0], recv.at[0], to), remote(srcu, dstu, send.at[1], recv.at[1], to))

    def a1_copy(b, k):
        return coded(code.at[b, k, 0], unit.at[b, k, 0], from_x.at[b, k], from_xu.at[b, k],
                     a1_send.at[b, k], a1_recv.at[b, k], (over_x, z))

    def b1_copy(b, k):
        return coded(code.at[b, k, 1], unit.at[b, k, 1], from_y.at[b, k], from_yu.at[b, k],
                     b1_send.at[b, k], b1_recv.at[b, k], (over_y, z))

    def a2_copy(b, k):
        return coded(code.at[b, k, 0], unit.at[b, k, 0], sum_y.at[k], sum_yu.at[k],
                     a2_send.at[k], a2_recv.at[k], (over_y, z))

    def b2_copy(b, k):
        return coded(code.at[b, k, 1], unit.at[b, k, 1], sum_x.at[k], sum_xu.at[k],
                     b2_send.at[k], b2_recv.at[k], (over_x, z))

    def share_copy(k):
        return remote(got.at[outer, k], rim.at[:, own_columns(k)], share_send.at[k], share_recv.at[k], (sib, z))

    def ra1_copy(j, k):
        return coded(rcode.at[j, k, 0], runit.at[j, k, 0], rfrom_x.at[j, k], rfrom_xu.at[j, k],
                     ra1_send.at[j, k], ra1_recv.at[j, k], (over_x, z))

    def rb1_copy(j, k):
        return coded(rcode.at[j, k, 1], runit.at[j, k, 1], rfrom_y.at[j, k], rfrom_yu.at[j, k],
                     rb1_send.at[j, k], rb1_recv.at[j, k], (over_y, z))

    def ra2_copy(j, k):
        return coded(rcode.at[j, k, 0], runit.at[j, k, 0], rsum_y.at[k], rsum_yu.at[k],
                     ra2_send.at[k], ra2_recv.at[k], (over_y, z))

    def rb2_copy(j, k):
        return coded(rcode.at[j, k, 1], runit.at[j, k, 1], rsum_x.at[k], rsum_xu.at[k],
                     rb2_send.at[k], rb2_recv.at[k], (over_x, z))

    def land_copy(k):
        return coded(ready.at[k], readyu.at[k], landed.at[k], landedu.at[k],
                     land_send.at[k], land_recv.at[k], (s, outer))

    def multiply(left, right):
        return lax.dot_general(left, right, (((0,), (0,)), ((), ())), preferred_element_type=jnp.float32)

    def encode(value, code_at, unit_at):
        top = jnp.maximum(jnp.max(jnp.abs(value), axis=0, keepdims=True), TINY)
        code_at[...] = jnp.round(value * (STEPS / top)).astype(jnp.int32).astype(jnp.int16)
        unit_at[...] = top * (1.0 / STEPS)

    def decode(codes, units):
        return codes.astype(jnp.int32).astype(jnp.float32) * units

    def stage(value, away_from_here, part_at, code_at, unit_at):
        @when(away_from_here)
        def _():
            encode(value, code_at, unit_at)

        @when(jnp.logical_not(away_from_here))
        def _():
            part_at[...] = value

    def relayed_block(j):
        return jnp.where(inside, z + orient * j, 0)

    def gathered(i):
        return both(inside, i == 3 * pieces - 1)

    def relay_product(j, k):
        b = relayed_block(j)
        far_x, far_y = apart(b)
        for side in range(2):
            stage(multiply(got[b, k], rim[:, side * half : (side + 1) * half]), (far_x, far_y)[side],
                  rpart.at[j, k, side], rcode.at[j, k, side], runit.at[j, k, side])

        @when(far_x)
        def _():
            ra1_copy(j, k).start()

        @when(far_y)
        def _():
            rb1_copy(j, k).start()

    def relay_combine(j, k):
        far_x, far_y = apart(relayed_block(j))

        @when(both(jnp.logical_not(far_x), far_y))
        def _():
            ra1_copy(j, k).wait_recv()
            encode(rpart[j, k, 0] + decode(rfrom_x[j, k], rfrom_xu[j, k]), rcode.at[j, k, 0], runit.at[j, k, 0])
            ra2_copy(j, k).start()

        @when(both(far_x, jnp.logical_not(far_y)))
        def _():
            rb1_copy(j, k).wait_recv()
            encode(rpart[j, k, 1] + decode(rfrom_y[j, k], rfrom_yu[j, k]), rcode.at[j, k, 1], runit.at[j, k, 1])
            rb2_copy(j, k).start()

    def product(i):
        away, k, sign, b, valid, second, relay = place(i)
        far_x, far_y = apart(b)
        passes = onward(away, k, sign, valid)

        @when(valid)
        def _():
            @when(away > 0)
            def _():
                for j in (core, 1 - core):
                    fwd_copy(b, k, j, sign).wait_recv()

                    @when(passes)
                    def _():
                        fwd_copy(b, k, j, sign).start()

                @when(both(inside, b == outer))
                def _():
                    share_copy(k).start()
                    rim[:, own_columns(k)] = got[b, k]

            for side in range(2):
                stage(multiply(got[b, k], feats[:, side * half : (side + 1) * half]), (far_x, far_y)[side],
                      part.at[b, k, side], code.at[b, k, side], unit.at[b, k, side])

            @when(far_x)
            def _():
                a1_copy(b, k).start()

            @when(far_y)
            def _():
                b1_copy(b, k).start()

        @when(gathered(i))
        def _():
            for p in range(pieces):
                share_copy(p).wait_recv()

            lax.fori_loop(0, near * (depth - 2), lambda m, _: (relay_product(m // near, lax.rem(m, near)), 0)[1], 0)

        @when(both(relay, k < relayed))
        def _():
            relay_product(depth - 2, k)

    home = (quad - z) * orient

    def hand_over(k):
        ra1_copy(home, k).wait_recv()
        ra2_copy(home, k).wait_recv()
        encode(rpart[home, k, 0] + decode(rfrom_x[home, k], rfrom_xu[home, k]) + decode(rsum_y[k], rsum_yu[k]),
               ready.at[k, :, 0:half], readyu.at[k, :, 0:half])
        rb1_copy(home, k).wait_recv()
        rb2_copy(home, k).wait_recv()
        encode(rpart[home, k, 1] + decode(rfrom_y[home, k], rfrom_yu[home, k]) + decode(rsum_x[k], rsum_xu[k]),
               ready.at[k, :, half : 2 * half], readyu.at[k, :, half : 2 * half])
        land_copy(k).start()

    def hand_over_early(i):
        @when(both(inside, quad != outer, home < depth - 2, i == base + 2))
        def _():
            lax.fori_loop(0, near, lambda k, _: (hand_over(k), 0)[1], 0)

        for k in range(relayed):
            @when(both(inside, home == depth - 2, i == base + 4 + 3 * k))
            def _():
                hand_over(k)

    def combine(i):
        _, k, _, b, valid, _, relay = place(i)
        far_x, far_y = apart(b)

        @when(both(valid, jnp.logical_not(far_x), far_y))
        def _():
            a1_copy(b, k).wait_recv()
            encode(part[b, k, 0] + decode(from_x[b, k], from_xu[b, k]), code.at[b, k, 0], unit.at[b, k, 0])
            a2_copy(b, k).start()

        @when(both(valid, far_x, jnp.logical_not(far_y)))
        def _():
            b1_copy(b, k).wait_recv()
            encode(part[b, k, 1] + decode(from_y[b, k], from_yu[b, k]), code.at[b, k, 1], unit.at[b, k, 1])
            b2_copy(b, k).start()

        @when(gathered(i))
        def _():
            lax.fori_loop(0, near * (depth - 2), lambda m, _: (relay_combine(m // near, lax.rem(m, near)), 0)[1], 0)

        @when(both(relay, k < relayed))
        def _():
            relay_combine(depth - 2, k)

    base = 3 * pieces

    def sent(k, _):
        for side in range(2):
            pair_copy(side * pieces + k, own_rows).wait_send()

        for j in range(2):
            @when(goes_up(k))
            def _():
                up_copy(k, j).wait_send()

            @when(goes_down(k))
            def _():
                down_copy(k, j).wait_send()

        @when(inside)
        def _():
            share_copy(k).wait_send()

        return 0

    def sent_late(i, _):
        away, k, sign, b, valid, _, relay = place(i)
        far_x, far_y = apart(b)

        @when(onward(away, k, sign, valid))
        def _():
            for j in range(2):
                fwd_copy(b, k, j, sign).wait_send()

        @when(both(valid, far_x))
        def _():
            a1_copy(b, k).wait_send()

        @when(both(valid, far_y))
        def _():
            b1_copy(b, k).wait_send()

        @when(both(valid, jnp.logical_not(far_x), far_y))
        def _():
            a2_copy(b, k).wait_send()

        @when(both(valid, far_x, jnp.logical_not(far_y)))
        def _():
            b2_copy(b, k).wait_send()

        return 0

    def main(i, _):
        @when(both(i >= base, lax.rem(i, 2) == 0))
        def _():
            combine(i - 2)
            combine(i - 1)

        hand_over_early(i)

        @when(both(i >= base, i < steps))
        def _():
            sent_late(i - base, 0)

        @when(both(i >= base, i < base + pieces))
        def _():
            sent(i - base, 0)

        @when(i < steps)
        def _():
            product(i)

        @when(both(i > pieces, i < base, lax.rem(i, 2) == 1))
        def _():
            combine((i - pieces) // 2)

            @when(i > pieces + 1)
            def _():
                combine(i - 3)
                combine(i - 2)

        return 0

    lax.fori_loop(0, steps + 1, main, 0)

    for step in range(1, peers):
        cnt_copy(step, lax.rem(s + peers - step, peers)).wait_recv()
    totals[s] = cnt_ref[...]
    token_total = jnp.sum(totals[...].astype(jnp.float32), axis=0)[0:1, :]
    scale = jnp.broadcast_to(jnp.concatenate([1.0 / token_total] * (half // LANES), axis=1), (LANES, half))

    def local(k):
        return either(inside, k >= quota(jnp.abs(quad - z)), quad == z)

    def finish(k, _):
        at = pl.ds(pl.multiple_of(k * LANES, LANES), LANES)

        @when(local(k))
        def _():
            a1_copy(quad, k).wait_recv()
            a2_copy(quad, k).wait_recv()
            o_ref[at, 0:half] = (part[quad, k, 0] + decode(from_x[quad, k], from_xu[quad, k])
                                 + decode(sum_y[k], sum_yu[k])) * scale
            b1_copy(quad, k).wait_recv()
            b2_copy(quad, k).wait_recv()
            o_ref[at, half : 2 * half] = (part[quad, k, 1] + decode(from_y[quad, k], from_yu[quad, k])
                                          + decode(sum_x[k], sum_xu[k])) * scale

        return 0

    lax.fori_loop(0, pieces, finish, 0)

    def take(k, _):
        at = pl.ds(pl.multiple_of(k * LANES, LANES), LANES)

        @when(both(on_rim, quad != z, k < quota(jnp.abs(quad - z))))
        def _():
            land_copy(k).wait_recv()
            for side in range(2):
                cols = slice(side * half, (side + 1) * half)
                o_ref[at, cols] = decode(landed[k, :, cols], landedu[k, :, cols]) * scale

        return 0

    lax.fori_loop(0, relayed, take, 0)

    @when(s < peers - 1)
    def _():
        halo.wait_send()

    for step in range(1, peers):
        cnt_copy(step, s).wait_send()

    lax.fori_loop(steps - base, steps, sent_late, 0)

    def sent_relayed(m, _):
        j, k = m // relayed, lax.rem(m, relayed)
        far_x, far_y = apart(relayed_block(j))
        live = both(inside, k < quota(j + 1))

        @when(both(live, far_x))
        def _():
            ra1_copy(j, k).wait_send()

        @when(both(live, far_y))
        def _():
            rb1_copy(j, k).wait_send()

        @when(both(live, jnp.logical_not(far_x), far_y))
        def _():
            ra2_copy(j, k).wait_send()

        @when(both(live, far_x, jnp.logical_not(far_y)))
        def _():
            rb2_copy(j, k).wait_send()

        @when(both(live, j == home))
        def _():
            land_copy(k).wait_send()

        return 0

    lax.fori_loop(0, relayed * (depth - 1), sent_relayed, 0)


def fused_on_device(peers, depth, inputs, conv_weight, conv_bias, doc_start, counts):
    rows, width = inputs.shape
    taps = conv_weight.shape[0]
    half = width // 2
    pieces = half // LANES
    relayed = pieces // 2
    vmem = pl.BlockSpec(memory_space=pltpu.VMEM)
    dma = lambda *shape: pltpu.SemaphoreType.DMA(shape)
    f32, i16 = jnp.float32, jnp.int16
    grid = (depth, pieces)
    outs = (depth - 1, relayed)
    return pl.pallas_call(
        functools.partial(gram_kernel, peers, depth, taps, 1, relayed),
        out_shape=jax.ShapeDtypeStruct((half, width), f32),
        in_specs=[pl.BlockSpec(memory_space=pl.ANY), vmem, vmem, vmem, pl.BlockSpec(memory_space=pltpu.SMEM)],
        out_specs=vmem,
        scratch_shapes=[
            pltpu.VMEM((rows + HALO, width), inputs.dtype),
            pltpu.VMEM((2 * rows, width), inputs.dtype),
            pltpu.VMEM((depth, pieces, 2 * rows, LANES), inputs.dtype),
            pltpu.VMEM((depth, pieces, 2, LANES, half), f32),
            pltpu.VMEM((depth, pieces, LANES, half), i16),
            pltpu.VMEM((depth, pieces, LANES, half), i16),
            pltpu.VMEM((pieces, LANES, half), i16),
            pltpu.VMEM((pieces, LANES, half), i16),
            pltpu.VMEM((2 * rows, width), inputs.dtype),
            pltpu.VMEM((*outs, 2, LANES, half), f32),
            pltpu.VMEM((*outs, LANES, half), i16),
            pltpu.VMEM((*outs, LANES, half), i16),
            pltpu.VMEM((relayed, LANES, half), i16),
            pltpu.VMEM((relayed, LANES, half), i16),
            pltpu.VMEM((relayed, LANES, width), i16),
            pltpu.VMEM((relayed, 1, width), f32),
            pltpu.VMEM((relayed, LANES, width), i16),
            pltpu.VMEM((relayed, 1, width), f32),
            pltpu.VMEM((peers, 8, LANES), jnp.int32),
            pltpu.VMEM((rows, LANES), jnp.int32),
            pltpu.VMEM((8, LANES), jnp.int32),
            pltpu.VMEM((width // LANES, LANES), f32),
            pltpu.VMEM((*grid, 2, LANES, half), i16),
            pltpu.VMEM((*grid, 2, 1, half), f32),
            pltpu.VMEM((*grid, 1, half), f32),
            pltpu.VMEM((*grid, 1, half), f32),
            pltpu.VMEM((pieces, 1, half), f32),
            pltpu.VMEM((pieces, 1, half), f32),
            pltpu.VMEM((*outs, 2, LANES, half), i16),
            pltpu.VMEM((*outs, 2, 1, half), f32),
            pltpu.VMEM((*outs, 1, half), f32),
            pltpu.VMEM((*outs, 1, half), f32),
            pltpu.VMEM((relayed, 1, half), f32),
            pltpu.VMEM((relayed, 1, half), f32),
            pltpu.SemaphoreType.DMA, dma(2), dma(peers), dma(peers), dma(2 * pieces), dma(2 * pieces),
            dma(pieces, 2), dma(pieces, 2), dma(*grid, 2), dma(*grid, 2),
            dma(*grid, 2), dma(*grid, 2), dma(*grid, 2), dma(*grid, 2),
            dma(pieces, 2), dma(pieces, 2), dma(pieces, 2), dma(pieces, 2),
            dma(pieces), dma(pieces), dma(*outs, 2), dma(*outs, 2), dma(*outs, 2), dma(*outs, 2),
            dma(relayed, 2), dma(relayed, 2), dma(relayed, 2), dma(relayed, 2), dma(relayed, 2), dma(relayed, 2),
        ],
        compiler_params=pltpu.CompilerParams(collective_id=0, has_side_effects=True,
                                             vmem_limit_bytes=63 * 1024 * 1024),
        name="gram",
    )(inputs, conv_weight, conv_bias.reshape(width // LANES, LANES), doc_start.reshape(rows // LANES, LANES), counts)


def passed_along(x, axis, by):
    peers = lax.axis_size(axis)
    pairs = [(i, i + by) for i in range(peers) if 0 <= i + by < peers]
    return lax.ppermute(x, axis, pairs)


def causal_conv(extended, weights, bias, position, doc_start, length):
    kernel_len = weights.shape[0]
    summed = jnp.zeros((length, weights.shape[1]), jnp.float32) + bias.astype(jnp.float32)
    for lag in range(kernel_len):
        window = extended[kernel_len - 1 - lag : kernel_len - 1 - lag + length].astype(jnp.float32)
        usable = position - lag >= doc_start
        summed = summed + jnp.where(usable[:, None], weights[lag].astype(jnp.float32) * window, 0.0)
    return jax.nn.silu(summed).astype(jnp.bfloat16)


def on_device(inputs, conv_weight, conv_bias, doc_start, counts):
    row_count = inputs.shape[0]
    kernel_len = conv_weight.shape[0]
    position = lax.axis_index("seq") * row_count + jnp.arange(row_count, dtype=jnp.int32)
    counted = jnp.arange(row_count, dtype=jnp.int32) < counts[0]
    token_total = lax.psum(counts.astype(jnp.float32)[0], "seq")
    prior = passed_along(inputs[row_count - (kernel_len - 1) :], "seq", 1)
    extended = jnp.concatenate([prior, inputs], axis=0)
    own_feats = causal_conv(extended, conv_weight, conv_bias, position, doc_start, row_count)
    kept = jnp.where(counted[:, None], own_feats, jnp.zeros_like(own_feats))
    whole = lax.all_gather(own_feats, "mp", axis=1, tiled=True)
    summed = lax.psum_scatter(
        lax.dot_general(whole, kept, (((0,), (0,)), ((), ())), preferred_element_type=jnp.float32),
        "seq",
        scatter_dimension=0,
        tiled=True,
    )
    return summed / token_total


def solution(mesh):
    placed = (P("seq", "mp"), P(None, "mp"), P("mp"), P("seq"), P("seq"))
    peers, depth = mesh.shape["seq"], mesh.shape["mp"]
    fits = peers == 2 * depth and depth == 2**2
    body = functools.partial(fused_on_device, peers, depth) if fits else on_device
    return jax.shard_map(body, mesh=mesh, in_specs=placed, out_specs=P("seq", "mp"), check_vma=False)
```

```python
import functools

import jax
import jax.numpy as jnp
from jax import lax
from jax.experimental import pallas as pl
from jax.experimental.pallas import tpu as pltpu
from jax.sharding import PartitionSpec as P

MESH = pl.DeviceIdType.MESH
LANES = 128
HALO = 16


def when(cond):
    return pl.when(cond)


TINY = 1e-30
STEPS = 32767.0


class Group:
    def __init__(self, *copies):
        self.copies = copies

    def start(self):
        for copy in self.copies:
            copy.start()

    def wait_send(self):
        for copy in self.copies:
            copy.wait_send()

    def wait_recv(self):
        for copy in self.copies:
            copy.wait_recv()


def gram_kernel(peers, depth, taps, near, relayed, x_hbm, taps_ref, bias_ref, doc_ref, counts_ref, o_ref, ext, feats, got, part,
                from_x, from_y, sum_y, sum_x, rim, rpart, rfrom_x, rfrom_y, rsum_y, rsum_x, ready, readyu, landed, landedu, totals,
                lag_ref, cnt_ref, bias_rows, code, unit, from_xu, from_yu, sum_yu, sum_xu, rcode, runit, rfrom_xu, rfrom_yu, rsum_yu, rsum_xu,
                load_sem, halo_sem, cnt_send, cnt_recv, pair_send, pair_recv,
                up_send, down_send, fwd_send, got_recv,
                a1_send, a1_recv, b1_send, b1_recv, a2_send, a2_recv, b2_send, b2_recv,
                share_send, share_recv, ra1_send, ra1_recv, rb1_send, rb1_recv,
                ra2_send, ra2_recv, rb2_send, rb2_recv, land_send, land_recv):
    s, z = lax.axis_index("seq"), lax.axis_index("mp")
    core, x, y = lax.rem(s, 2), lax.rem(s // 2, 2), s // 4
    sib, over_x, over_y = s + 1 - 2 * core, s + 2 - 4 * x, s + 4 - 8 * y
    quad = s // 2
    rows, width = x_hbm.shape
    half = width // 2
    pieces = half // LANES
    on_rim = jnp.logical_or(z == 0, z == depth - 1)
    inside = jnp.logical_not(on_rim)
    orient = jnp.where(z < depth // 2, 1, -1)
    outer = jnp.where(z < depth // 2, 0, depth - 1)

    def remote(src, dst, send, recv, to):
        return pltpu.make_async_remote_copy(src_ref=src, dst_ref=dst, send_sem=send, recv_sem=recv,
                                            device_id=to, device_id_type=MESH)

    def both(*conds):
        return functools.reduce(jnp.logical_and, conds)

    def either(*conds):
        return functools.reduce(jnp.logical_or, conds)

    load = pltpu.make_async_copy(x_hbm, ext.at[pl.ds(HALO, rows)], load_sem)
    load.start()

    barrier = pltpu.get_barrier_semaphore()
    for step in range(1, peers):
        pl.semaphore_signal(barrier, inc=1, device_id=(lax.rem(s + step, peers), z), device_id_type=MESH)

    @when(z > 0)
    def _():
        pl.semaphore_signal(barrier, inc=1, device_id=(s, z - 1), device_id_type=MESH)

    @when(z < depth - 1)
    def _():
        pl.semaphore_signal(barrier, inc=1, device_id=(s, z + 1), device_id_type=MESH)

    bias_rows[...] = bias_ref[...].astype(jnp.float32)
    cnt_ref[...] = jnp.broadcast_to(counts_ref[0], cnt_ref.shape)
    block = LANES

    def mark_block(r, _):
        first = pl.multiple_of(r * block, block)
        within = first + lax.broadcasted_iota(jnp.int32, (block, LANES), 0)
        start = jnp.transpose(jnp.broadcast_to(doc_ref[pl.ds(r, 1), :], (block, LANES)))
        reach = jnp.minimum(s * rows + within - start, taps - 1)
        lag_ref[pl.ds(first, block), :] = reach + jnp.where(within < counts_ref[0], taps, 0)
        return 0

    lax.fori_loop(0, rows // block, mark_block, 0)

    load.wait()
    pl.semaphore_wait(barrier, peers - 1 + jnp.where(z > 0, 1, 0) + jnp.where(z < depth - 1, 1, 0))

    halo = remote(ext.at[pl.ds(rows, HALO)], ext.at[pl.ds(0, HALO)], halo_sem.at[0], halo_sem.at[1],
                  (lax.rem(s + 1, peers), z))

    @when(s < peers - 1)
    def _():
        halo.start()

    def cnt_copy(step, slot):
        return remote(cnt_ref, totals.at[slot], cnt_send.at[step], cnt_recv.at[slot],
                      (lax.rem(s + step, peers), z))

    for step in range(1, peers):
        cnt_copy(step, s).start()

    own_rows = pl.multiple_of(core * rows, rows)

    def conv(column, low, high):
        at = pl.ds(pl.multiple_of(column, LANES), LANES)
        taps_here = taps_ref[:, at].astype(jnp.float32)
        bias_here = bias_rows[pl.ds(column // LANES, 1), :]

        def body(r, _):
            first = pl.multiple_of(r * block, block)
            seen = ext[pl.ds(first, block + HALO), at].astype(jnp.float32)
            mark = lag_ref[pl.ds(first, block), :]
            lags = jnp.bitwise_and(mark, taps - 1)
            total = jnp.broadcast_to(bias_here, (block, LANES))
            for lag_ in range(taps):
                window = (pltpu.roll(seen, lag_, 0) if lag_ else seen)[HALO:]
                term = jnp.broadcast_to(taps_here[lag_ : lag_ + 1], (block, LANES)) * window
                total = total + jnp.where(lags >= lag_, term, 0.0)
            value = total / (1.0 + jnp.exp(-total))
            value = jnp.where(mark >= taps, value, 0.0)
            feats[pl.ds(pl.multiple_of(own_rows + first, block), block), at] = value.astype(feats.dtype)
            return 0

        lax.fori_loop(low, high, body, 0)

    def pair_copy(piece, row0):
        spot = feats.at[pl.ds(row0, rows), pl.ds(pl.multiple_of(piece * LANES, LANES), LANES)]
        return remote(spot, spot, pair_send.at[piece], pair_recv.at[piece], (sib, z))

    def own_columns(k):
        return pl.ds(pl.multiple_of(core * half + k * LANES, LANES), LANES)

    def tokens(j):
        return pl.ds(pl.multiple_of(j * rows, rows), rows)

    def up_copy(k, j):
        return remote(feats.at[tokens(j), own_columns(k)], got.at[z, k, tokens(j)], up_send.at[k, j],
                      got_recv.at[z, k, j], (s, lax.rem(z + 1, depth)))

    def down_copy(k, j):
        return remote(feats.at[tokens(j), own_columns(k)], got.at[z, k, tokens(j)], down_send.at[k, j],
                      got_recv.at[z, k, j], (s, lax.rem(z + depth - 1, depth)))

    def goes_up(k):
        return either(z < depth - 2, both(z == depth - 2, k >= near))

    def goes_down(k):
        return either(z > 1, both(z == 1, k >= near))

    blocks = rows // block
    for side in (1 - core, core):
        conv(side * half, 1, blocks)

    @when(s == 0)
    def _():
        ext[0:HALO, :] = jnp.zeros((HALO, width), ext.dtype)

    @when(s > 0)
    def _():
        halo.wait_recv()

    def spread(k, _):
        def make(side):
            piece = side * pieces + k
            conv(piece * LANES, 0, jnp.where(k == 0, 1, blocks))
            pair_copy(piece, own_rows).start()


        def send(j):
            @when(goes_up(k))
            def _():
                up_copy(k, j).start()

            @when(goes_down(k))
            def _():
                down_copy(k, j).start()

        make(1 - core)
        make(core)
        send(core)
        pair_copy(core * pieces + k, own_rows).wait_recv()
        send(1 - core)
        return 0

    lax.fori_loop(0, pieces, spread, 0)

    def settle(k, _):
        pair_copy((1 - core) * pieces + k, own_rows).wait_recv()
        got[z, k] = feats[:, own_columns(k)]
        return 0

    lax.fori_loop(0, pieces, settle, 0)

    steps = pieces + 2 * pieces * (depth - 1)

    def quota(span):
        return jnp.where(span == depth - 1, relayed, near)

    def place(i):
        later = i - pieces
        own = i < pieces
        later = jnp.where(own, 0, later)
        away = jnp.where(own, 0, later // (2 * pieces) + 1)
        k = jnp.where(own, i, lax.rem(later, 2 * pieces) // 2)
        second = both(jnp.logical_not(own), lax.rem(later, 2) == 1)
        sign = jnp.where(second, -orient, orient)
        block_at = z + sign * away
        within = both(block_at >= 0, block_at < depth)
        block_in = jnp.where(within, block_at, 0)
        valid = both(within, either(own, inside, k >= quota(away)))
        relay = both(inside, away == 2, second)
        return away, k, sign, block_in, valid, second, relay

    def onward(away, k, sign, valid):
        beyond = z - sign
        deep = both(beyond > 0, beyond < depth - 1)
        edge = either(beyond == 0, beyond == depth - 1)
        return both(valid, away > 0, either(deep, both(edge, k >= quota(away + 1))))

    def apart(block_at):
        return lax.rem(block_at, 2) != x, block_at // 2 != y

    def fwd_copy(block_at, k, j, sign):
        to = lax.rem(z - sign + depth, depth)
        return remote(got.at[block_at, k, tokens(j)], got.at[block_at, k, tokens(j)], fwd_send.at[block_at, k, j],
                      got_recv.at[block_at, k, j], (s, to))

    def coded(src, srcu, dst, dstu, send, recv, to):
        return Group(remote(src, dst, send.at[0], recv.at[0], to), remote(srcu, dstu, send.at[1], recv.at[1], to))

    def a1_copy(b, k):
        return coded(code.at[b, k, 0], unit.at[b, k, 0], from_x.at[b // 2, k], from_xu.at[b // 2, k],
                     a1_send.at[b // 2, k], a1_recv.at[b // 2, k], (over_x, z))

    def b1_copy(b, k):
        return coded(code.at[b, k, 1], unit.at[b, k, 1], from_y.at[b % 2, k], from_yu.at[b % 2, k],
                     b1_send.at[b % 2, k], b1_recv.at[b % 2, k], (over_y, z))

    def a2_copy(b, k):
        return coded(code.at[b, k, 0], unit.at[b, k, 0], sum_y.at[k], sum_yu.at[k],
                     a2_send.at[k], a2_recv.at[k], (over_y, z))

    def b2_copy(b, k):
        return coded(code.at[b, k, 1], unit.at[b, k, 1], sum_x.at[k], sum_xu.at[k],
                     b2_send.at[k], b2_recv.at[k], (over_x, z))

    def share_copy(k):
        return remote(got.at[outer, k], rim.at[:, own_columns(k)], share_send.at[k], share_recv.at[k], (sib, z))

    def ra1_copy(j, k):
        return coded(rcode.at[j, k, 0], runit.at[j, k, 0], rfrom_x.at[relayed_block(j) // 2, k], rfrom_xu.at[relayed_block(j) // 2, k],
                     ra1_send.at[relayed_block(j) // 2, k], ra1_recv.at[relayed_block(j) // 2, k], (over_x, z))

    def rb1_copy(j, k):
        return coded(rcode.at[j, k, 1], runit.at[j, k, 1], rfrom_y.at[relayed_block(j) % 2, k], rfrom_yu.at[relayed_block(j) % 2, k],
                     rb1_send.at[relayed_block(j) % 2, k], rb1_recv.at[relayed_block(j) % 2, k], (over_y, z))

    def ra2_copy(j, k):
        return coded(rcode.at[j, k, 0], runit.at[j, k, 0], rsum_y.at[k], rsum_yu.at[k],
                     ra2_send.at[k], ra2_recv.at[k], (over_y, z))

    def rb2_copy(j, k):
        return coded(rcode.at[j, k, 1], runit.at[j, k, 1], rsum_x.at[k], rsum_xu.at[k],
                     rb2_send.at[k], rb2_recv.at[k], (over_x, z))

    def land_copy(k):
        return coded(ready.at[k], readyu.at[k], landed.at[k], landedu.at[k],
                     land_send.at[k], land_recv.at[k], (s, outer))

    def multiply(left, right):
        return lax.dot_general(left, right, (((0,), (0,)), ((), ())), preferred_element_type=jnp.float32)

    def encode(value, code_at, unit_at):
        top = jnp.maximum(jnp.max(jnp.abs(value), axis=0, keepdims=True), TINY)
        code_at[...] = jnp.round(value * (STEPS / top)).astype(jnp.int32).astype(jnp.int16)
        unit_at[...] = top * (1.0 / STEPS)

    def decode(codes, units):
        return codes.astype(jnp.int32).astype(jnp.float32) * units

    def stage(value, away_from_here, part_at, code_at, unit_at):
        @when(away_from_here)
        def _():
            encode(value, code_at, unit_at)

        @when(jnp.logical_not(away_from_here))
        def _():
            part_at[...] = value

    def relayed_block(j):
        return jnp.where(inside, z + orient * j, 0)

    def gathered(i):
        return both(inside, i == 3 * pieces - 1)

    def relay_product(j, k):
        b = relayed_block(j)
        far_x, far_y = apart(b)
        for side in range(2):
            stage(multiply(got[b, k], rim[:, side * half : (side + 1) * half]), (far_x, far_y)[side],
                  rpart.at[j, k, side], rcode.at[j, k, side], runit.at[j, k, side])

        @when(far_x)
        def _():
            ra1_copy(j, k).start()

        @when(far_y)
        def _():
            rb1_copy(j, k).start()

    def relay_combine(j, k):
        far_x, far_y = apart(relayed_block(j))

        @when(both(jnp.logical_not(far_x), far_y))
        def _():
            ra1_copy(j, k).wait_recv()
            encode(rpart[j, k, 0] + decode(rfrom_x[relayed_block(j) // 2, k], rfrom_xu[relayed_block(j) // 2, k]), rcode.at[j, k, 0], runit.at[j, k, 0])
            ra2_copy(j, k).start()

        @when(both(far_x, jnp.logical_not(far_y)))
        def _():
            rb1_copy(j, k).wait_recv()
            encode(rpart[j, k, 1] + decode(rfrom_y[relayed_block(j) % 2, k], rfrom_yu[relayed_block(j) % 2, k]), rcode.at[j, k, 1], runit.at[j, k, 1])
            rb2_copy(j, k).start()

    def product(i):
        away, k, sign, b, valid, second, relay = place(i)
        far_x, far_y = apart(b)
        passes = onward(away, k, sign, valid)

        @when(valid)
        def _():
            @when(away > 0)
            def _():
                for j in (core, 1 - core):
                    fwd_copy(b, k, j, sign).wait_recv()

                    @when(passes)
                    def _():
                        fwd_copy(b, k, j, sign).start()

                @when(both(inside, b == outer))
                def _():
                    share_copy(k).start()
                    rim[:, own_columns(k)] = got[b, k]

            @when(both(inside, away == 2, k < relayed))
            def _():
                relay_product(depth - 2, k)

            for side in range(2):
                stage(multiply(got[b, k], feats[:, side * half : (side + 1) * half]), (far_x, far_y)[side],
                      part.at[b, k, side], code.at[b, k, side], unit.at[b, k, side])

            @when(far_x)
            def _():
                a1_copy(b, k).start()

            @when(far_y)
            def _():
                b1_copy(b, k).start()

        @when(gathered(i))
        def _():
            for p in range(pieces):
                share_copy(p).wait_recv()

            lax.fori_loop(0, near * (depth - 2), lambda m, _: (relay_product(m // near, lax.rem(m, near)), 0)[1], 0)

    home = (quad - z) * orient

    def hand_over(k):
        ra1_copy(home, k).wait_recv()
        ra2_copy(home, k).wait_recv()
        encode(rpart[home, k, 0] + decode(rfrom_x[y, k], rfrom_xu[y, k]) + decode(rsum_y[k], rsum_yu[k]),
               ready.at[k, :, 0:half], readyu.at[k, :, 0:half])
        rb1_copy(home, k).wait_recv()
        rb2_copy(home, k).wait_recv()
        encode(rpart[home, k, 1] + decode(rfrom_y[x, k], rfrom_yu[x, k]) + decode(rsum_x[k], rsum_xu[k]),
               ready.at[k, :, half : 2 * half], readyu.at[k, :, half : 2 * half])
        land_copy(k).start()

    def hand_over_early(i):
        @when(both(inside, quad != outer, home < depth - 2, i == base + 2))
        def _():
            lax.fori_loop(0, near, lambda k, _: (hand_over(k), 0)[1], 0)

        for k in range(relayed):
            @when(both(inside, home == depth - 2, i == base + 4 + 3 * k))
            def _():
                hand_over(k)

    def combine(i):
        _, k, _, b, valid, _, relay = place(i)
        far_x, far_y = apart(b)

        @when(both(valid, jnp.logical_not(far_x), far_y))
        def _():
            a1_copy(b, k).wait_recv()
            encode(part[b, k, 0] + decode(from_x[b // 2, k], from_xu[b // 2, k]), code.at[b, k, 0], unit.at[b, k, 0])
            a2_copy(b, k).start()

        @when(both(valid, far_x, jnp.logical_not(far_y)))
        def _():
            b1_copy(b, k).wait_recv()
            encode(part[b, k, 1] + decode(from_y[b % 2, k], from_yu[b % 2, k]), code.at[b, k, 1], unit.at[b, k, 1])
            b2_copy(b, k).start()

        @when(gathered(i))
        def _():
            lax.fori_loop(0, near * (depth - 2), lambda m, _: (relay_combine(m // near, lax.rem(m, near)), 0)[1], 0)

        @when(both(relay, k < relayed))
        def _():
            relay_combine(depth - 2, k)

    base = 3 * pieces

    def sent(k, _):
        for side in range(2):
            pair_copy(side * pieces + k, own_rows).wait_send()

        for j in range(2):
            @when(goes_up(k))
            def _():
                up_copy(k, j).wait_send()

            @when(goes_down(k))
            def _():
                down_copy(k, j).wait_send()

        @when(inside)
        def _():
            share_copy(k).wait_send()

        return 0

    def sent_late(i, _):
        away, k, sign, b, valid, _, relay = place(i)
        far_x, far_y = apart(b)

        @when(onward(away, k, sign, valid))
        def _():
            for j in range(2):
                fwd_copy(b, k, j, sign).wait_send()

        @when(both(valid, far_x))
        def _():
            a1_copy(b, k).wait_send()

        @when(both(valid, far_y))
        def _():
            b1_copy(b, k).wait_send()

        @when(both(valid, jnp.logical_not(far_x), far_y))
        def _():
            a2_copy(b, k).wait_send()

        @when(both(valid, far_x, jnp.logical_not(far_y)))
        def _():
            b2_copy(b, k).wait_send()

        return 0

    def main(i, _):
        @when(both(i >= base, lax.rem(i, 2) == 0))
        def _():
            combine(i - 1)
            combine(i - 2)

        hand_over_early(i)

        @when(both(i >= base, i < steps))
        def _():
            sent_late(i - base, 0)

        @when(both(i >= base, i < base + pieces))
        def _():
            sent(i - base, 0)

        @when(i < steps)
        def _():
            product(i)

        @when(both(i > pieces, i < base, lax.rem(i, 2) == 1))
        def _():
            combine((i - pieces) // 2)

            @when(i > pieces + 1)
            def _():
                combine(i - 3)
                combine(i - 2)

        return 0

    lax.fori_loop(0, steps + 1, main, 0)

    for step in range(1, peers):
        cnt_copy(step, lax.rem(s + peers - step, peers)).wait_recv()
    totals[s] = cnt_ref[...]
    token_total = jnp.sum(totals[...].astype(jnp.float32), axis=0)[0:1, :]
    scale = jnp.broadcast_to(jnp.concatenate([1.0 / token_total] * (half // LANES), axis=1), (LANES, half))

    def local(k):
        return either(inside, k >= quota(jnp.abs(quad - z)), quad == z)

    def finish(k, _):
        at = pl.ds(pl.multiple_of(k * LANES, LANES), LANES)

        @when(local(k))
        def _():
            a1_copy(quad, k).wait_recv()
            a2_copy(quad, k).wait_recv()
            o_ref[at, 0:half] = (part[quad, k, 0] + decode(from_x[y, k], from_xu[y, k])
                                 + decode(sum_y[k], sum_yu[k])) * scale
            b1_copy(quad, k).wait_recv()
            b2_copy(quad, k).wait_recv()
            o_ref[at, half : 2 * half] = (part[quad, k, 1] + decode(from_y[x, k], from_yu[x, k])
                                          + decode(sum_x[k], sum_xu[k])) * scale

        return 0

    lax.fori_loop(0, pieces, finish, 0)

    def take(k, _):
        at = pl.ds(pl.multiple_of(k * LANES, LANES), LANES)

        @when(both(on_rim, quad != z, k < quota(jnp.abs(quad - z))))
        def _():
            land_copy(k).wait_recv()
            for side in range(2):
                cols = slice(side * half, (side + 1) * half)
                o_ref[at, cols] = decode(landed[k, :, cols], landedu[k, :, cols]) * scale

        return 0

    lax.fori_loop(0, relayed, take, 0)

    @when(s < peers - 1)
    def _():
        halo.wait_send()

    for step in range(1, peers):
        cnt_copy(step, s).wait_send()

    lax.fori_loop(steps - base, steps, sent_late, 0)

    def sent_relayed(m, _):
        j, k = m // relayed, lax.rem(m, relayed)
        far_x, far_y = apart(relayed_block(j))
        live = both(inside, k < quota(j + 1))

        @when(both(live, far_x))
        def _():
            ra1_copy(j, k).wait_send()

        @when(both(live, far_y))
        def _():
            rb1_copy(j, k).wait_send()

        @when(both(live, jnp.logical_not(far_x), far_y))
        def _():
            ra2_copy(j, k).wait_send()

        @when(both(live, far_x, jnp.logical_not(far_y)))
        def _():
            rb2_copy(j, k).wait_send()

        @when(both(live, j == home))
        def _():
            land_copy(k).wait_send()

        return 0

    lax.fori_loop(0, relayed * (depth - 1), sent_relayed, 0)


def fused_on_device(peers, depth, inputs, conv_weight, conv_bias, doc_start, counts):
    rows, width = inputs.shape
    taps = conv_weight.shape[0]
    half = width // 2
    pieces = half // LANES
    relayed = pieces // 2
    vmem = pl.BlockSpec(memory_space=pltpu.VMEM)
    dma = lambda *shape: pltpu.SemaphoreType.DMA(shape)
    f32, i16 = jnp.float32, jnp.int16
    grid = (depth, pieces)
    outs = (depth - 1, relayed)
    return pl.pallas_call(
        functools.partial(gram_kernel, peers, depth, taps, 1, relayed),
        out_shape=jax.ShapeDtypeStruct((half, width), f32),
        in_specs=[pl.BlockSpec(memory_space=pl.ANY), vmem, vmem, vmem, pl.BlockSpec(memory_space=pltpu.SMEM)],
        out_specs=vmem,
        scratch_shapes=[
            pltpu.VMEM((rows + HALO, width), inputs.dtype),
            pltpu.VMEM((2 * rows, width), inputs.dtype),
            pltpu.VMEM((depth, pieces, 2 * rows, LANES), inputs.dtype),
            pltpu.VMEM((depth, pieces, 2, LANES, half), f32),
            pltpu.VMEM((2, pieces, LANES, half), i16),
            pltpu.VMEM((2, pieces, LANES, half), i16),
            pltpu.VMEM((pieces, LANES, half), i16),
            pltpu.VMEM((pieces, LANES, half), i16),
            pltpu.VMEM((2 * rows, width), inputs.dtype),
            pltpu.VMEM((*outs, 2, LANES, half), f32),
            pltpu.VMEM((2, relayed, LANES, half), i16),
            pltpu.VMEM((2, relayed, LANES, half), i16),
            pltpu.VMEM((relayed, LANES, half), i16),
            pltpu.VMEM((relayed, LANES, half), i16),
            pltpu.VMEM((relayed, LANES, width), i16),
            pltpu.VMEM((relayed, 1, width), f32),
            pltpu.VMEM((relayed, LANES, width), i16),
            pltpu.VMEM((relayed, 1, width), f32),
            pltpu.VMEM((peers, 8, LANES), jnp.int32),
            pltpu.VMEM((rows, LANES), jnp.int32),
            pltpu.VMEM((8, LANES), jnp.int32),
            pltpu.VMEM((width // LANES, LANES), f32),
            pltpu.VMEM((*grid, 2, LANES, half), i16),
            pltpu.VMEM((*grid, 2, 1, half), f32),
            pltpu.VMEM((2, pieces, 1, half), f32),
            pltpu.VMEM((2, pieces, 1, half), f32),
            pltpu.VMEM((pieces, 1, half), f32),
            pltpu.VMEM((pieces, 1, half), f32),
            pltpu.VMEM((*outs, 2, LANES, half), i16),
            pltpu.VMEM((*outs, 2, 1, half), f32),
            pltpu.VMEM((2, relayed, 1, half), f32),
            pltpu.VMEM((2, relayed, 1, half), f32),
            pltpu.VMEM((relayed, 1, half), f32),
            pltpu.VMEM((relayed, 1, half), f32),
            pltpu.SemaphoreType.DMA, dma(2), dma(peers), dma(peers), dma(2 * pieces), dma(2 * pieces),
            dma(pieces, 2), dma(pieces, 2), dma(*grid, 2), dma(*grid, 2),
            dma(2, pieces, 2), dma(2, pieces, 2), dma(2, pieces, 2), dma(2, pieces, 2),
            dma(pieces, 2), dma(pieces, 2), dma(pieces, 2), dma(pieces, 2),
            dma(pieces), dma(pieces),
            dma(2, relayed, 2), dma(2, relayed, 2), dma(2, relayed, 2), dma(2, relayed, 2),
            dma(relayed, 2), dma(relayed, 2), dma(relayed, 2), dma(relayed, 2), dma(relayed, 2), dma(relayed, 2),
        ],
        compiler_params=pltpu.CompilerParams(collective_id=0, has_side_effects=True,
                                             vmem_limit_bytes=52480 * 1024),
        name="gram",
    )(inputs, conv_weight, conv_bias.reshape(width // LANES, LANES), doc_start.reshape(rows // LANES, LANES), counts)


def passed_along(x, axis, by):
    peers = lax.axis_size(axis)
    pairs = [(i, i + by) for i in range(peers) if 0 <= i + by < peers]
    return lax.ppermute(x, axis, pairs)


def causal_conv(extended, weights, bias, position, doc_start, length):
    kernel_len = weights.shape[0]
    summed = jnp.zeros((length, weights.shape[1]), jnp.float32) + bias.astype(jnp.float32)
    for lag in range(kernel_len):
        window = extended[kernel_len - 1 - lag : kernel_len - 1 - lag + length].astype(jnp.float32)
        usable = position - lag >= doc_start
        summed = summed + jnp.where(usable[:, None], weights[lag].astype(jnp.float32) * window, 0.0)
    return jax.nn.silu(summed).astype(jnp.bfloat16)


def on_device(inputs, conv_weight, conv_bias, doc_start, counts):
    row_count = inputs.shape[0]
    kernel_len = conv_weight.shape[0]
    position = lax.axis_index("seq") * row_count + jnp.arange(row_count, dtype=jnp.int32)
    counted = jnp.arange(row_count, dtype=jnp.int32) < counts[0]
    token_total = lax.psum(counts.astype(jnp.float32)[0], "seq")
    prior = passed_along(inputs[row_count - (kernel_len - 1) :], "seq", 1)
    extended = jnp.concatenate([prior, inputs], axis=0)
    own_feats = causal_conv(extended, conv_weight, conv_bias, position, doc_start, row_count)
    kept = jnp.where(counted[:, None], own_feats, jnp.zeros_like(own_feats))
    whole = lax.all_gather(own_feats, "mp", axis=1, tiled=True)
    summed = lax.psum_scatter(
        lax.dot_general(whole, kept, (((0,), (0,)), ((), ())), preferred_element_type=jnp.float32),
        "seq",
        scatter_dimension=0,
        tiled=True,
    )
    return summed / token_total


def solution(mesh):
    placed = (P("seq", "mp"), P(None, "mp"), P("mp"), P("seq"), P("seq"))
    peers, depth = mesh.shape["seq"], mesh.shape["mp"]
    fits = peers == 2 * depth and depth == 2**2
    body = functools.partial(fused_on_device, peers, depth) if fits else on_device
    return jax.shard_map(body, mesh=mesh, in_specs=placed, out_specs=P("seq", "mp"), check_vma=False)
```

```python
import functools

import jax
import jax.numpy as jnp
from jax import lax
from jax.experimental import pallas as pl
from jax.experimental.pallas import tpu as pltpu
from jax.sharding import PartitionSpec as P

MESH = pl.DeviceIdType.MESH
LANES = 128
HALO = 16


def when(cond):
    return pl.when(cond)


TINY = 1e-30
STEPS = 32767.0


class Group:
    def __init__(self, *copies):
        self.copies = copies

    def start(self):
        for copy in self.copies:
            copy.start()

    def wait_send(self):
        for copy in self.copies:
            copy.wait_send()

    def wait_recv(self):
        for copy in self.copies:
            copy.wait_recv()


def gram_kernel(peers, depth, taps, near, relayed, x_hbm, taps_hbm, bias_hbm, doc_hbm, counts_ref, o_ref, ext, feats, got, part,
                from_x, from_y, sum_y, sum_x, rim, rpart, rfrom_x, rfrom_y, rsum_y, rsum_x, ready, readyu, landed, landedu, totals,
                lag_ref, cnt_ref, bias_rows, taps_ref, bias_ref, doc_ref, small_sem, code, unit, from_xu, from_yu, sum_yu, sum_xu, rcode, runit, rfrom_xu, rfrom_yu, rsum_yu, rsum_xu,
                load_sem, halo_sem, cnt_send, cnt_recv, pair_send, pair_recv,
                up_send, down_send, fwd_send, got_recv,
                a1_send, a1_recv, b1_send, b1_recv, a2_send, a2_recv, b2_send, b2_recv,
                share_send, share_recv, ra1_send, ra1_recv, rb1_send, rb1_recv,
                ra2_send, ra2_recv, rb2_send, rb2_recv, land_send, land_recv):
    s, z = lax.axis_index("seq"), lax.axis_index("mp")
    core, x, y = lax.rem(s, 2), lax.rem(s // 2, 2), s // 4
    sib, over_x, over_y = s + 1 - 2 * core, s + 2 - 4 * x, s + 4 - 8 * y
    quad = s // 2
    rows, width = x_hbm.shape
    half = width // 2
    pieces = half // LANES
    on_rim = jnp.logical_or(z == 0, z == depth - 1)
    inside = jnp.logical_not(on_rim)
    orient = jnp.where(z < depth // 2, 1, -1)
    outer = jnp.where(z < depth // 2, 0, depth - 1)

    def remote(src, dst, send, recv, to):
        return pltpu.make_async_remote_copy(src_ref=src, dst_ref=dst, send_sem=send, recv_sem=recv,
                                            device_id=to, device_id_type=MESH)

    def both(*conds):
        return functools.reduce(jnp.logical_and, conds)

    def either(*conds):
        return functools.reduce(jnp.logical_or, conds)

    load = pltpu.make_async_copy(x_hbm, ext.at[pl.ds(HALO, rows)], load_sem)
    load.start()
    small = [pltpu.make_async_copy(src, dst, small_sem.at[n]) for n, (src, dst) in
             enumerate(((doc_hbm, doc_ref), (bias_hbm, bias_ref), (taps_hbm, taps_ref)))]
    for copy in small:
        copy.start()

    barrier = pltpu.get_barrier_semaphore()
    for step in range(1, peers):
        pl.semaphore_signal(barrier, inc=1, device_id=(lax.rem(s + step, peers), z), device_id_type=MESH)

    @when(z > 0)
    def _():
        pl.semaphore_signal(barrier, inc=1, device_id=(s, z - 1), device_id_type=MESH)

    @when(z < depth - 1)
    def _():
        pl.semaphore_signal(barrier, inc=1, device_id=(s, z + 1), device_id_type=MESH)

    for copy in small:
        copy.wait()

    bias_rows[...] = bias_ref[...].astype(jnp.float32)
    cnt_ref[...] = jnp.broadcast_to(counts_ref[0], cnt_ref.shape)
    block = LANES

    def mark_block(r, _):
        first = pl.multiple_of(r * block, block)
        within = first + lax.broadcasted_iota(jnp.int32, (block, LANES), 0)
        start = jnp.transpose(jnp.broadcast_to(doc_ref[pl.ds(r, 1), :], (block, LANES)))
        reach = jnp.minimum(s * rows + within - start, taps - 1)
        lag_ref[pl.ds(first, block), :] = reach + jnp.where(within < counts_ref[0], taps, 0)
        return 0

    lax.fori_loop(0, rows // block, mark_block, 0)

    load.wait()
    pl.semaphore_wait(barrier, peers - 1 + jnp.where(z > 0, 1, 0) + jnp.where(z < depth - 1, 1, 0))

    halo = remote(ext.at[pl.ds(rows, HALO)], ext.at[pl.ds(0, HALO)], halo_sem.at[0], halo_sem.at[1],
                  (lax.rem(s + 1, peers), z))

    @when(s < peers - 1)
    def _():
        halo.start()

    def cnt_copy(step, slot):
        return remote(cnt_ref, totals.at[slot], cnt_send.at[step], cnt_recv.at[slot],
                      (lax.rem(s + step, peers), z))

    for step in range(1, peers):
        cnt_copy(step, s).start()

    own_rows = pl.multiple_of(core * rows, rows)

    def conv(column, low, high):
        at = pl.ds(pl.multiple_of(column, LANES), LANES)
        taps_here = taps_ref[:, at].astype(jnp.float32)
        bias_here = bias_rows[pl.ds(column // LANES, 1), :]

        def body(r, _):
            first = pl.multiple_of(r * block, block)
            seen = ext[pl.ds(first, block + HALO), at].astype(jnp.float32)
            mark = lag_ref[pl.ds(first, block), :]
            lags = jnp.bitwise_and(mark, taps - 1)
            total = jnp.broadcast_to(bias_here, (block, LANES))
            for lag_ in range(taps):
                window = (pltpu.roll(seen, lag_, 0) if lag_ else seen)[HALO:]
                term = jnp.broadcast_to(taps_here[lag_ : lag_ + 1], (block, LANES)) * window
                total = total + jnp.where(lags >= lag_, term, 0.0)
            value = total / (1.0 + jnp.exp(-total))
            value = jnp.where(mark >= taps, value, 0.0)
            feats[pl.ds(pl.multiple_of(own_rows + first, block), block), at] = value.astype(feats.dtype)
            return 0

        lax.fori_loop(low, high, body, 0)

    def pair_copy(piece, row0):
        spot = feats.at[pl.ds(row0, rows), pl.ds(pl.multiple_of(piece * LANES, LANES), LANES)]
        return remote(spot, spot, pair_send.at[piece], pair_recv.at[piece], (sib, z))

    def own_columns(k):
        return pl.ds(pl.multiple_of(core * half + k * LANES, LANES), LANES)

    def tokens(j):
        return pl.ds(pl.multiple_of(j * rows, rows), rows)

    def up_copy(k, j):
        return remote(feats.at[tokens(j), own_columns(k)], got.at[z, k, tokens(j)], up_send.at[k, j],
                      got_recv.at[z, k, j], (s, lax.rem(z + 1, depth)))

    def down_copy(k, j):
        return remote(feats.at[tokens(j), own_columns(k)], got.at[z, k, tokens(j)], down_send.at[k, j],
                      got_recv.at[z, k, j], (s, lax.rem(z + depth - 1, depth)))

    def goes_up(k):
        return either(z < depth - 2, both(z == depth - 2, k >= near))

    def goes_down(k):
        return either(z > 1, both(z == 1, k >= near))

    blocks = rows // block
    for side in (1 - core, core):
        conv(side * half, 1, blocks)

    @when(s == 0)
    def _():
        ext[0:HALO, :] = jnp.zeros((HALO, width), ext.dtype)

    @when(s > 0)
    def _():
        halo.wait_recv()

    def spread(k, _):
        def make(side):
            piece = side * pieces + k
            conv(piece * LANES, 0, jnp.where(k == 0, 1, blocks))
            pair_copy(piece, own_rows).start()


        def send(j):
            @when(goes_up(k))
            def _():
                up_copy(k, j).start()

            @when(goes_down(k))
            def _():
                down_copy(k, j).start()

        make(1 - core)
        make(core)
        send(core)
        pair_copy(core * pieces + k, own_rows).wait_recv()
        send(1 - core)
        return 0

    lax.fori_loop(0, pieces, spread, 0)

    def settle(k, _):
        pair_copy((1 - core) * pieces + k, own_rows).wait_recv()
        got[z, k] = feats[:, own_columns(k)]
        return 0

    lax.fori_loop(0, pieces, settle, 0)

    steps = pieces + 2 * pieces * (depth - 1)

    def quota(span):
        return jnp.where(span == depth - 1, relayed, near)

    def place(i):
        later = i - pieces
        own = i < pieces
        later = jnp.where(own, 0, later)
        away = jnp.where(own, 0, later // (2 * pieces) + 1)
        k = jnp.where(own, i, lax.rem(later, 2 * pieces) // 2)
        second = both(jnp.logical_not(own), lax.rem(later, 2) == 1)
        sign = jnp.where(second, -orient, orient)
        block_at = z + sign * away
        within = both(block_at >= 0, block_at < depth)
        block_in = jnp.where(within, block_at, 0)
        valid = both(within, either(own, inside, k >= quota(away)))
        relay = both(inside, away == 2, second)
        return away, k, sign, block_in, valid, second, relay

    def onward(away, k, sign, valid):
        beyond = z - sign
        deep = both(beyond > 0, beyond < depth - 1)
        edge = either(beyond == 0, beyond == depth - 1)
        return both(valid, away > 0, either(deep, both(edge, k >= quota(away + 1))))

    def apart(block_at):
        return lax.rem(block_at, 2) != x, block_at // 2 != y

    def fwd_copy(block_at, k, j, sign):
        to = lax.rem(z - sign + depth, depth)
        return remote(got.at[block_at, k, tokens(j)], got.at[block_at, k, tokens(j)], fwd_send.at[block_at, k, j],
                      got_recv.at[block_at, k, j], (s, to))

    def coded(src, srcu, dst, dstu, send, recv, to):
        return Group(remote(src, dst, send.at[0], recv.at[0], to), remote(srcu, dstu, send.at[1], recv.at[1], to))

    def a1_copy(b, k):
        return coded(code.at[b, k, 0], unit.at[b, k, 0], from_x.at[b // 2, k], from_xu.at[b // 2, k],
                     a1_send.at[b // 2, k], a1_recv.at[b // 2, k], (over_x, z))

    def b1_copy(b, k):
        return coded(code.at[b, k, 1], unit.at[b, k, 1], from_y.at[b % 2, k], from_yu.at[b % 2, k],
                     b1_send.at[b % 2, k], b1_recv.at[b % 2, k], (over_y, z))

    def a2_copy(b, k):
        return coded(code.at[b, k, 0], unit.at[b, k, 0], sum_y.at[k], sum_yu.at[k],
                     a2_send.at[k], a2_recv.at[k], (over_y, z))

    def b2_copy(b, k):
        return coded(code.at[b, k, 1], unit.at[b, k, 1], sum_x.at[k], sum_xu.at[k],
                     b2_send.at[k], b2_recv.at[k], (over_x, z))

    def share_copy(k):
        return remote(got.at[outer, k], rim.at[:, own_columns(k)], share_send.at[k], share_recv.at[k], (sib, z))

    def ra1_copy(j, k):
        return coded(rcode.at[j, k, 0], runit.at[j, k, 0], rfrom_x.at[relayed_block(j) // 2, k], rfrom_xu.at[relayed_block(j) // 2, k],
                     ra1_send.at[relayed_block(j) // 2, k], ra1_recv.at[relayed_block(j) // 2, k], (over_x, z))

    def rb1_copy(j, k):
        return coded(rcode.at[j, k, 1], runit.at[j, k, 1], rfrom_y.at[relayed_block(j) % 2, k], rfrom_yu.at[relayed_block(j) % 2, k],
                     rb1_send.at[relayed_block(j) % 2, k], rb1_recv.at[relayed_block(j) % 2, k], (over_y, z))

    def ra2_copy(j, k):
        return coded(rcode.at[j, k, 0], runit.at[j, k, 0], rsum_y.at[k], rsum_yu.at[k],
                     ra2_send.at[k], ra2_recv.at[k], (over_y, z))

    def rb2_copy(j, k):
        return coded(rcode.at[j, k, 1], runit.at[j, k, 1], rsum_x.at[k], rsum_xu.at[k],
                     rb2_send.at[k], rb2_recv.at[k], (over_x, z))

    def land_copy(k):
        return coded(ready.at[k], readyu.at[k], landed.at[k], landedu.at[k],
                     land_send.at[k], land_recv.at[k], (s, outer))

    def multiply(left, right):
        return lax.dot_general(left, right, (((0,), (0,)), ((), ())), preferred_element_type=jnp.float32)

    def encode(value, code_at, unit_at):
        top = jnp.maximum(jnp.max(jnp.abs(value), axis=0, keepdims=True), TINY)
        code_at[...] = jnp.round(value * (STEPS / top)).astype(jnp.int32).astype(jnp.int16)
        unit_at[...] = top * (1.0 / STEPS)

    def decode(codes, units):
        return codes.astype(jnp.int32).astype(jnp.float32) * units

    def stage(value, away_from_here, part_at, code_at, unit_at):
        @when(away_from_here)
        def _():
            encode(value, code_at, unit_at)

        @when(jnp.logical_not(away_from_here))
        def _():
            part_at[...] = value

    def relayed_block(j):
        return jnp.where(inside, z + orient * j, 0)

    def gathered(i):
        return both(inside, i == 3 * pieces - 1)

    def relay_product(j, k):
        b = relayed_block(j)
        far_x, far_y = apart(b)
        for side in range(2):
            stage(multiply(got[b, k], rim[:, side * half : (side + 1) * half]), (far_x, far_y)[side],
                  rpart.at[j, k, side], rcode.at[j, k, side], runit.at[j, k, side])

        @when(far_x)
        def _():
            ra1_copy(j, k).start()

        @when(far_y)
        def _():
            rb1_copy(j, k).start()

    def relay_combine(j, k):
        far_x, far_y = apart(relayed_block(j))

        @when(both(jnp.logical_not(far_x), far_y))
        def _():
            ra1_copy(j, k).wait_recv()
            encode(rpart[j, k, 0] + decode(rfrom_x[relayed_block(j) // 2, k], rfrom_xu[relayed_block(j) // 2, k]), rcode.at[j, k, 0], runit.at[j, k, 0])
            ra2_copy(j, k).start()

        @when(both(far_x, jnp.logical_not(far_y)))
        def _():
            rb1_copy(j, k).wait_recv()
            encode(rpart[j, k, 1] + decode(rfrom_y[relayed_block(j) % 2, k], rfrom_yu[relayed_block(j) % 2, k]), rcode.at[j, k, 1], runit.at[j, k, 1])
            rb2_copy(j, k).start()

    def product(i):
        away, k, sign, b, valid, second, relay = place(i)
        far_x, far_y = apart(b)
        passes = onward(away, k, sign, valid)

        @when(valid)
        def _():
            @when(away > 0)
            def _():
                for j in (core, 1 - core):
                    fwd_copy(b, k, j, sign).wait_recv()

                    @when(passes)
                    def _():
                        fwd_copy(b, k, j, sign).start()

                @when(both(inside, b == outer))
                def _():
                    share_copy(k).start()
                    rim[:, own_columns(k)] = got[b, k]

            @when(both(inside, away == 2, k < relayed))
            def _():
                relay_product(depth - 2, k)

            for side in range(2):
                stage(multiply(got[b, k], feats[:, side * half : (side + 1) * half]), (far_x, far_y)[side],
                      part.at[b, k, side], code.at[b, k, side], unit.at[b, k, side])

            @when(far_x)
            def _():
                a1_copy(b, k).start()

            @when(far_y)
            def _():
                b1_copy(b, k).start()

        @when(gathered(i))
        def _():
            for p in range(pieces):
                share_copy(p).wait_recv()

            lax.fori_loop(0, near * (depth - 2), lambda m, _: (relay_product(m // near, lax.rem(m, near)), 0)[1], 0)

    home = (quad - z) * orient

    def hand_over(k):
        ra1_copy(home, k).wait_recv()
        ra2_copy(home, k).wait_recv()
        encode(rpart[home, k, 0] + decode(rfrom_x[y, k], rfrom_xu[y, k]) + decode(rsum_y[k], rsum_yu[k]),
               ready.at[k, :, 0:half], readyu.at[k, :, 0:half])
        rb1_copy(home, k).wait_recv()
        rb2_copy(home, k).wait_recv()
        encode(rpart[home, k, 1] + decode(rfrom_y[x, k], rfrom_yu[x, k]) + decode(rsum_x[k], rsum_xu[k]),
               ready.at[k, :, half : 2 * half], readyu.at[k, :, half : 2 * half])
        land_copy(k).start()

    def hand_over_early(i):
        @when(both(inside, quad != outer, home < depth - 2, i == base + 2))
        def _():
            lax.fori_loop(0, near, lambda k, _: (hand_over(k), 0)[1], 0)

        for k in range(relayed):
            @when(both(inside, home == depth - 2, i == base + (2, 7)[k]))
            def _():
                hand_over(k)

    def combine(i):
        _, k, _, b, valid, _, relay = place(i)
        far_x, far_y = apart(b)

        @when(both(valid, jnp.logical_not(far_x), far_y))
        def _():
            a1_copy(b, k).wait_recv()
            encode(part[b, k, 0] + decode(from_x[b // 2, k], from_xu[b // 2, k]), code.at[b, k, 0], unit.at[b, k, 0])
            a2_copy(b, k).start()

        @when(both(valid, far_x, jnp.logical_not(far_y)))
        def _():
            b1_copy(b, k).wait_recv()
            encode(part[b, k, 1] + decode(from_y[b % 2, k], from_yu[b % 2, k]), code.at[b, k, 1], unit.at[b, k, 1])
            b2_copy(b, k).start()

        @when(gathered(i))
        def _():
            lax.fori_loop(0, near * (depth - 2), lambda m, _: (relay_combine(m // near, lax.rem(m, near)), 0)[1], 0)

        @when(both(relay, k < relayed))
        def _():
            relay_combine(depth - 2, k)

    base = 3 * pieces

    def sent(k, _):
        for side in range(2):
            pair_copy(side * pieces + k, own_rows).wait_send()

        for j in range(2):
            @when(goes_up(k))
            def _():
                up_copy(k, j).wait_send()

            @when(goes_down(k))
            def _():
                down_copy(k, j).wait_send()

        @when(inside)
        def _():
            share_copy(k).wait_send()

        return 0

    def sent_late(i, _):
        away, k, sign, b, valid, _, relay = place(i)
        far_x, far_y = apart(b)

        @when(onward(away, k, sign, valid))
        def _():
            for j in range(2):
                fwd_copy(b, k, j, sign).wait_send()

        @when(both(valid, far_x))
        def _():
            a1_copy(b, k).wait_send()

        @when(both(valid, far_y))
        def _():
            b1_copy(b, k).wait_send()

        @when(both(valid, jnp.logical_not(far_x), far_y))
        def _():
            a2_copy(b, k).wait_send()

        @when(both(valid, far_x, jnp.logical_not(far_y)))
        def _():
            b2_copy(b, k).wait_send()

        return 0

    def main(i, _):
        @when(both(i >= base, lax.rem(i, 2) == 0))
        def _():
            combine(i - 1)
            combine(i - 2)

        hand_over_early(i)

        @when(both(i >= base, i < steps))
        def _():
            sent_late(i - base, 0)

        @when(both(i >= base, i < base + pieces))
        def _():
            sent(i - base, 0)

        @when(i < steps)
        def _():
            product(i)

        @when(both(i > pieces, i < base, lax.rem(i, 2) == 1))
        def _():
            combine((i - pieces) // 2)

            @when(i > pieces + 1)
            def _():
                combine(i - 3)
                combine(i - 2)

        return 0

    lax.fori_loop(0, steps + 1, main, 0)

    for step in range(1, peers):
        cnt_copy(step, lax.rem(s + peers - step, peers)).wait_recv()
    totals[s] = cnt_ref[...]
    token_total = jnp.sum(totals[...].astype(jnp.float32), axis=0)[0:1, :]
    scale = jnp.broadcast_to(jnp.concatenate([1.0 / token_total] * (half // LANES), axis=1), (LANES, half))

    def local(k):
        return either(inside, k >= quota(jnp.abs(quad - z)), quad == z)

    def finish(k, _):
        at = pl.ds(pl.multiple_of(k * LANES, LANES), LANES)

        @when(local(k))
        def _():
            a1_copy(quad, k).wait_recv()
            a2_copy(quad, k).wait_recv()
            o_ref[at, 0:half] = (part[quad, k, 0] + decode(from_x[y, k], from_xu[y, k])
                                 + decode(sum_y[k], sum_yu[k])) * scale
            b1_copy(quad, k).wait_recv()
            b2_copy(quad, k).wait_recv()
            o_ref[at, half : 2 * half] = (part[quad, k, 1] + decode(from_y[x, k], from_yu[x, k])
                                          + decode(sum_x[k], sum_xu[k])) * scale

        return 0

    lax.fori_loop(0, pieces, finish, 0)

    def take(k, _):
        at = pl.ds(pl.multiple_of(k * LANES, LANES), LANES)

        @when(both(on_rim, quad != z, k < quota(jnp.abs(quad - z))))
        def _():
            land_copy(k).wait_recv()
            for side in range(2):
                cols = slice(side * half, (side + 1) * half)
                o_ref[at, cols] = decode(landed[k, :, cols], landedu[k, :, cols]) * scale

        return 0

    lax.fori_loop(0, relayed, take, 0)

    @when(s < peers - 1)
    def _():
        halo.wait_send()

    for step in range(1, peers):
        cnt_copy(step, s).wait_send()

    lax.fori_loop((steps - base) // 2, steps // 2, lambda n, _: sent_late(2 * n, 0), 0)

    def sent_relayed(m, _):
        j, k = m // relayed, lax.rem(m, relayed)
        far_x, far_y = apart(relayed_block(j))
        live = both(inside, k < quota(j + 1))

        @when(both(live, far_x))
        def _():
            ra1_copy(j, k).wait_send()

        @when(both(live, far_y))
        def _():
            rb1_copy(j, k).wait_send()

        @when(both(live, jnp.logical_not(far_x), far_y))
        def _():
            ra2_copy(j, k).wait_send()

        @when(both(live, far_x, jnp.logical_not(far_y)))
        def _():
            rb2_copy(j, k).wait_send()

        @when(both(live, j == home))
        def _():
            land_copy(k).wait_send()

        return 0

    @when(inside)
    def _():
        lax.fori_loop(0, relayed * (depth - 1), sent_relayed, 0)


def fused_on_device(peers, depth, inputs, conv_weight, conv_bias, doc_start, counts):
    rows, width = inputs.shape
    taps = conv_weight.shape[0]
    half = width // 2
    pieces = half // LANES
    relayed = pieces // 2
    vmem = pl.BlockSpec(memory_space=pltpu.VMEM)
    dma = lambda *shape: pltpu.SemaphoreType.DMA(shape)
    f32, i16 = jnp.float32, jnp.int16
    grid = (depth, pieces)
    outs = (depth - 1, relayed)
    return pl.pallas_call(
        functools.partial(gram_kernel, peers, depth, taps, 1, relayed),
        out_shape=jax.ShapeDtypeStruct((half, width), f32),
        in_specs=[pl.BlockSpec(memory_space=pl.ANY)] * 4 + [ pl.BlockSpec(memory_space=pltpu.SMEM)],
        out_specs=vmem,
        scratch_shapes=[
            pltpu.VMEM((rows + HALO, width), inputs.dtype),
            pltpu.VMEM((2 * rows, width), inputs.dtype),
            pltpu.VMEM((depth, pieces, 2 * rows, LANES), inputs.dtype),
            pltpu.VMEM((depth, pieces, 2, LANES, half), f32),
            pltpu.VMEM((2, pieces, LANES, half), i16),
            pltpu.VMEM((2, pieces, LANES, half), i16),
            pltpu.VMEM((pieces, LANES, half), i16),
            pltpu.VMEM((pieces, LANES, half), i16),
            pltpu.VMEM((2 * rows, width), inputs.dtype),
            pltpu.VMEM((*outs, 2, LANES, half), f32),
            pltpu.VMEM((2, relayed, LANES, half), i16),
            pltpu.VMEM((2, relayed, LANES, half), i16),
            pltpu.VMEM((relayed, LANES, half), i16),
            pltpu.VMEM((relayed, LANES, half), i16),
            pltpu.VMEM((relayed, LANES, width), i16),
            pltpu.VMEM((relayed, 1, width), f32),
            pltpu.VMEM((relayed, LANES, width), i16),
            pltpu.VMEM((relayed, 1, width), f32),
            pltpu.VMEM((peers, 8, LANES), jnp.int32),
            pltpu.VMEM((rows, LANES), jnp.int32),
            pltpu.VMEM((8, LANES), jnp.int32),
            pltpu.VMEM((width // LANES, LANES), f32),
            pltpu.VMEM(conv_weight.shape, conv_weight.dtype),
            pltpu.VMEM((width // LANES, LANES), conv_bias.dtype),
            pltpu.VMEM((rows // LANES, LANES), doc_start.dtype),
            dma(3),
            pltpu.VMEM((*grid, 2, LANES, half), i16),
            pltpu.VMEM((*grid, 2, 1, half), f32),
            pltpu.VMEM((2, pieces, 1, half), f32),
            pltpu.VMEM((2, pieces, 1, half), f32),
            pltpu.VMEM((pieces, 1, half), f32),
            pltpu.VMEM((pieces, 1, half), f32),
            pltpu.VMEM((*outs, 2, LANES, half), i16),
            pltpu.VMEM((*outs, 2, 1, half), f32),
            pltpu.VMEM((2, relayed, 1, half), f32),
            pltpu.VMEM((2, relayed, 1, half), f32),
            pltpu.VMEM((relayed, 1, half), f32),
            pltpu.VMEM((relayed, 1, half), f32),
            pltpu.SemaphoreType.DMA, dma(2), dma(peers), dma(peers), dma(2 * pieces), dma(2 * pieces),
            dma(pieces, 2), dma(pieces, 2), dma(*grid, 2), dma(*grid, 2),
            dma(2, pieces, 2), dma(2, pieces, 2), dma(2, pieces, 2), dma(2, pieces, 2),
            dma(pieces, 2), dma(pieces, 2), dma(pieces, 2), dma(pieces, 2),
            dma(pieces), dma(pieces),
            dma(2, relayed, 2), dma(2, relayed, 2), dma(2, relayed, 2), dma(2, relayed, 2),
            dma(relayed, 2), dma(relayed, 2), dma(relayed, 2), dma(relayed, 2), dma(relayed, 2), dma(relayed, 2),
        ],
        compiler_params=pltpu.CompilerParams(collective_id=0, has_side_effects=True,
                                             vmem_limit_bytes=52480 * 1024),
        name="gram",
    )(inputs, *(pltpu.with_memory_space_constraint(a, pltpu.HBM) for a in (conv_weight, conv_bias.reshape(width // LANES, LANES), doc_start.reshape(rows // LANES, LANES))), counts)


def passed_along(x, axis, by):
    peers = lax.axis_size(axis)
    pairs = [(i, i + by) for i in range(peers) if 0 <= i + by < peers]
    return lax.ppermute(x, axis, pairs)


def causal_conv(extended, weights, bias, position, doc_start, length):
    kernel_len = weights.shape[0]
    summed = jnp.zeros((length, weights.shape[1]), jnp.float32) + bias.astype(jnp.float32)
    for lag in range(kernel_len):
        window = extended[kernel_len - 1 - lag : kernel_len - 1 - lag + length].astype(jnp.float32)
        usable = position - lag >= doc_start
        summed = summed + jnp.where(usable[:, None], weights[lag].astype(jnp.float32) * window, 0.0)
    return jax.nn.silu(summed).astype(jnp.bfloat16)


def on_device(inputs, conv_weight, conv_bias, doc_start, counts):
    row_count = inputs.shape[0]
    kernel_len = conv_weight.shape[0]
    position = lax.axis_index("seq") * row_count + jnp.arange(row_count, dtype=jnp.int32)
    counted = jnp.arange(row_count, dtype=jnp.int32) < counts[0]
    token_total = lax.psum(counts.astype(jnp.float32)[0], "seq")
    prior = passed_along(inputs[row_count - (kernel_len - 1) :], "seq", 1)
    extended = jnp.concatenate([prior, inputs], axis=0)
    own_feats = causal_conv(extended, conv_weight, conv_bias, position, doc_start, row_count)
    kept = jnp.where(counted[:, None], own_feats, jnp.zeros_like(own_feats))
    whole = lax.all_gather(own_feats, "mp", axis=1, tiled=True)
    summed = lax.psum_scatter(
        lax.dot_general(whole, kept, (((0,), (0,)), ((), ())), preferred_element_type=jnp.float32),
        "seq",
        scatter_dimension=0,
        tiled=True,
    )
    return summed / token_total


def solution(mesh):
    placed = (P("seq", "mp"), P(None, "mp"), P("mp"), P("seq"), P("seq"))
    peers, depth = mesh.shape["seq"], mesh.shape["mp"]
    fits = peers == 2 * depth and depth == 2**2
    body = functools.partial(fused_on_device, peers, depth) if fits else on_device
    return jax.shard_map(body, mesh=mesh, in_specs=placed, out_specs=P("seq", "mp"), check_vma=False)
```

```python
import functools

import jax
import jax.numpy as jnp
from jax import lax
from jax.experimental import pallas as pl
from jax.experimental.pallas import tpu as pltpu
from jax.sharding import PartitionSpec as P

MESH = pl.DeviceIdType.MESH
LANES = 128
HALO = 16


def when(cond):
    return pl.when(cond)


TINY = 1e-30
STEPS = 32767.0


class Group:
    def __init__(self, *copies):
        self.copies = copies

    def start(self):
        for copy in self.copies:
            copy.start()

    def wait_send(self):
        for copy in self.copies:
            copy.wait_send()

    def wait_recv(self):
        for copy in self.copies:
            copy.wait_recv()


def gram_kernel(peers, depth, taps, near, relayed, x_hbm, taps_hbm, bias_hbm, doc_hbm, counts_ref, o_ref, ext, feats, got, part,
                from_x, from_y, sum_y, sum_x, rim, rpart, rfrom_x, rfrom_y, rsum_y, rsum_x, ready, readyu, landed, landedu, totals,
                lag_ref, cnt_ref, bias_rows, taps_ref, bias_ref, doc_ref, small_sem, code, unit, from_xu, from_yu, sum_yu, sum_xu, rcode, runit, rfrom_xu, rfrom_yu, rsum_yu, rsum_xu,
                load_sem, halo_sem, cnt_send, cnt_recv, pair_send, pair_recv,
                up_send, down_send, fwd_send, got_recv,
                a1_send, a1_recv, b1_send, b1_recv, a2_send, a2_recv, b2_send, b2_recv,
                share_send, share_recv, ra1_send, ra1_recv, rb1_send, rb1_recv,
                ra2_send, ra2_recv, rb2_send, rb2_recv, land_send, land_recv):
    s, z = lax.axis_index("seq"), lax.axis_index("mp")
    core, x, y = lax.rem(s, 2), lax.rem(s // 2, 2), s // 4
    sib, over_x, over_y = s + 1 - 2 * core, s + 2 - 4 * x, s + 4 - 8 * y
    quad = s // 2
    rows, width = x_hbm.shape
    half = width // 2
    pieces = half // LANES
    on_rim = jnp.logical_or(z == 0, z == depth - 1)
    inside = jnp.logical_not(on_rim)
    orient = jnp.where(z < depth // 2, 1, -1)
    outer = jnp.where(z < depth // 2, 0, depth - 1)

    def remote(src, dst, send, recv, to):
        return pltpu.make_async_remote_copy(src_ref=src, dst_ref=dst, send_sem=send, recv_sem=recv,
                                            device_id=to, device_id_type=MESH)

    def both(*conds):
        return functools.reduce(jnp.logical_and, conds)

    def either(*conds):
        return functools.reduce(jnp.logical_or, conds)

    load = pltpu.make_async_copy(x_hbm, ext.at[pl.ds(HALO, rows)], load_sem)
    load.start()
    small = [pltpu.make_async_copy(src, dst, small_sem.at[n]) for n, (src, dst) in
             enumerate(((doc_hbm, doc_ref), (bias_hbm, bias_ref), (taps_hbm, taps_ref)))]
    for copy in small:
        copy.start()

    barrier = pltpu.get_barrier_semaphore()
    for step in range(1, peers):
        pl.semaphore_signal(barrier, inc=1, device_id=(lax.rem(s + step, peers), z), device_id_type=MESH)

    @when(z > 0)
    def _():
        pl.semaphore_signal(barrier, inc=1, device_id=(s, z - 1), device_id_type=MESH)

    @when(z < depth - 1)
    def _():
        pl.semaphore_signal(barrier, inc=1, device_id=(s, z + 1), device_id_type=MESH)

    for copy in small:
        copy.wait()

    bias_rows[...] = bias_ref[...].astype(jnp.float32)
    cnt_ref[...] = jnp.broadcast_to(counts_ref[0], cnt_ref.shape)
    block = LANES

    def mark_block(r, _):
        first = pl.multiple_of(r * block, block)
        within = first + lax.broadcasted_iota(jnp.int32, (block, LANES), 0)
        start = jnp.transpose(jnp.broadcast_to(doc_ref[pl.ds(r, 1), :], (block, LANES)))
        reach = jnp.minimum(s * rows + within - start, taps - 1)
        lag_ref[pl.ds(first, block), :] = reach + jnp.where(within < counts_ref[0], taps, 0)
        return 0

    lax.fori_loop(0, rows // block, mark_block, 0)

    load.wait()
    pl.semaphore_wait(barrier, peers - 1 + jnp.where(z > 0, 1, 0) + jnp.where(z < depth - 1, 1, 0))

    halo = remote(ext.at[pl.ds(rows, HALO)], ext.at[pl.ds(0, HALO)], halo_sem.at[0], halo_sem.at[1],
                  (lax.rem(s + 1, peers), z))

    @when(s < peers - 1)
    def _():
        halo.start()

    def cnt_copy(step, slot):
        return remote(cnt_ref, totals.at[slot], cnt_send.at[step], cnt_recv.at[slot],
                      (lax.rem(s + step, peers), z))

    for step in range(1, peers):
        cnt_copy(step, s).start()

    own_rows = pl.multiple_of(core * rows, rows)

    def conv(column, low, high):
        at = pl.ds(pl.multiple_of(column, LANES), LANES)
        taps_here = taps_ref[:, at].astype(jnp.float32)
        bias_here = bias_rows[pl.ds(column // LANES, 1), :]

        def body(r, _):
            first = pl.multiple_of(r * block, block)
            seen = ext[pl.ds(first, block + HALO), at].astype(jnp.float32)
            mark = lag_ref[pl.ds(first, block), :]
            lags = jnp.bitwise_and(mark, taps - 1)
            total = jnp.broadcast_to(bias_here, (block, LANES))
            for lag_ in range(taps):
                window = (pltpu.roll(seen, lag_, 0) if lag_ else seen)[HALO:]
                term = jnp.broadcast_to(taps_here[lag_ : lag_ + 1], (block, LANES)) * window
                total = total + jnp.where(lags >= lag_, term, 0.0)
            value = total / (1.0 + jnp.exp(-total))
            value = jnp.where(mark >= taps, value, 0.0)
            feats[pl.ds(pl.multiple_of(own_rows + first, block), block), at] = value.astype(feats.dtype)
            return 0

        lax.fori_loop(low, high, body, 0)

    def pair_copy(piece, row0):
        spot = feats.at[pl.ds(row0, rows), pl.ds(pl.multiple_of(piece * LANES, LANES), LANES)]
        return remote(spot, spot, pair_send.at[piece], pair_recv.at[piece], (sib, z))

    def own_columns(k):
        return pl.ds(pl.multiple_of(core * half + k * LANES, LANES), LANES)

    def tokens(j):
        return pl.ds(pl.multiple_of(j * (rows // 2), rows // 2), rows // 2)

    def chunks(of):
        return 2 * of, 2 * of + 1

    def up_copy(k, j):
        return remote(feats.at[tokens(j), own_columns(k)], got.at[z, k, tokens(j)], up_send.at[k],
                      got_recv.at[z, k, j], (s, lax.rem(z + 1, depth)))

    def down_copy(k, j):
        return remote(feats.at[tokens(j), own_columns(k)], got.at[z, k, tokens(j)], down_send.at[k],
                      got_recv.at[z, k, j], (s, lax.rem(z + depth - 1, depth)))

    def piece_sent(k, send):
        remote(got.at[z, k], got.at[z, k], send, got_recv.at[z, k, 0], (s, lax.rem(z + 1, depth))).wait_send()

    def goes_up(k):
        return either(z < depth - 2, both(z == depth - 2, k >= near))

    def goes_down(k):
        return either(z > 1, both(z == 1, k >= near))

    blocks = rows // block
    conv(core * half, 1, blocks)

    @when(goes_up(0))
    def _():
        up_copy(0, 2 * core + 1).start()

    @when(goes_down(0))
    def _():
        down_copy(0, 2 * core + 1).start()

    conv((1 - core) * half, 1, blocks)

    @when(s == 0)
    def _():
        ext[0:HALO, :] = jnp.zeros((HALO, width), ext.dtype)

    @when(s > 0)
    def _():
        halo.wait_recv()

    def spread(k, _):
        def make(side):
            piece = side * pieces + k
            conv(piece * LANES, 0, jnp.where(k == 0, 1, blocks))
            pair_copy(piece, own_rows).start()


        def send(of):
            for n, j in enumerate(chunks(of)):
                due = either(k > 0, of != core) if n else True

                @when(both(goes_up(k), due))
                def _():
                    up_copy(k, j).start()

                @when(both(goes_down(k), due))
                def _():
                    down_copy(k, j).start()

        make(1 - core)
        make(core)
        send(core)
        pair_copy(core * pieces + k, own_rows).wait_recv()
        send(1 - core)
        return 0

    lax.fori_loop(0, pieces, spread, 0)

    def settle(k, _):
        pair_copy((1 - core) * pieces + k, own_rows).wait_recv()
        got[z, k] = feats[:, own_columns(k)]
        return 0

    lax.fori_loop(0, pieces, settle, 0)

    steps = pieces + 2 * pieces * (depth - 1)

    def quota(span):
        return jnp.where(span == depth - 1, relayed, near)

    def place(i):
        later = i - pieces
        own = i < pieces
        later = jnp.where(own, 0, later)
        away = jnp.where(own, 0, later // (2 * pieces) + 1)
        k = jnp.where(own, i, lax.rem(later, 2 * pieces) // 2)
        second = both(jnp.logical_not(own), lax.rem(later, 2) == 1)
        sign = jnp.where(second, -orient, orient)
        block_at = z + sign * away
        within = both(block_at >= 0, block_at < depth)
        block_in = jnp.where(within, block_at, 0)
        valid = both(within, either(own, inside, k >= quota(away)))
        relay = both(inside, away == 2, second)
        return away, k, sign, block_in, valid, second, relay

    def onward(away, k, sign, valid):
        beyond = z - sign
        deep = both(beyond > 0, beyond < depth - 1)
        edge = either(beyond == 0, beyond == depth - 1)
        return both(valid, away > 0, either(deep, both(edge, k >= quota(away + 1))))

    def apart(block_at):
        return lax.rem(block_at, 2) != x, block_at // 2 != y

    def fwd_copy(block_at, k, j, sign):
        to = lax.rem(z - sign + depth, depth)
        return remote(got.at[block_at, k, tokens(j)], got.at[block_at, k, tokens(j)], fwd_send.at[block_at, k],
                      got_recv.at[block_at, k, j], (s, to))

    def coded(src, srcu, dst, dstu, send, recv, to):
        return Group(remote(src, dst, send.at[0], recv.at[0], to), remote(srcu, dstu, send.at[1], recv.at[1], to))

    def a1_copy(b, k):
        return coded(code.at[b, k, 0], unit.at[b, k, 0], from_x.at[b // 2, k], from_xu.at[b // 2, k],
                     a1_send.at[b // 2, k], a1_recv.at[b // 2, k], (over_x, z))

    def b1_copy(b, k):
        return coded(code.at[b, k, 1], unit.at[b, k, 1], from_y.at[b % 2, k], from_yu.at[b % 2, k],
                     b1_send.at[b % 2, k], b1_recv.at[b % 2, k], (over_y, z))

    def a2_copy(b, k):
        return coded(code.at[b, k, 0], unit.at[b, k, 0], sum_y.at[k], sum_yu.at[k],
                     a2_send.at[k], a2_recv.at[k], (over_y, z))

    def b2_copy(b, k):
        return coded(code.at[b, k, 1], unit.at[b, k, 1], sum_x.at[k], sum_xu.at[k],
                     b2_send.at[k], b2_recv.at[k], (over_x, z))

    def share_copy(k):
        return remote(got.at[outer, k], rim.at[:, own_columns(k)], share_send.at[k], share_recv.at[k], (sib, z))

    def ra1_copy(j, k):
        return coded(rcode.at[j, k, 0], runit.at[j, k, 0], rfrom_x.at[relayed_block(j) // 2, k], rfrom_xu.at[relayed_block(j) // 2, k],
                     ra1_send.at[relayed_block(j) // 2, k], ra1_recv.at[relayed_block(j) // 2, k], (over_x, z))

    def rb1_copy(j, k):
        return coded(rcode.at[j, k, 1], runit.at[j, k, 1], rfrom_y.at[relayed_block(j) % 2, k], rfrom_yu.at[relayed_block(j) % 2, k],
                     rb1_send.at[relayed_block(j) % 2, k], rb1_recv.at[relayed_block(j) % 2, k], (over_y, z))

    def ra2_copy(j, k):
        return coded(rcode.at[j, k, 0], runit.at[j, k, 0], rsum_y.at[k], rsum_yu.at[k],
                     ra2_send.at[k], ra2_recv.at[k], (over_y, z))

    def rb2_copy(j, k):
        return coded(rcode.at[j, k, 1], runit.at[j, k, 1], rsum_x.at[k], rsum_xu.at[k],
                     rb2_send.at[k], rb2_recv.at[k], (over_x, z))

    def land_copy(k):
        return coded(ready.at[k], readyu.at[k], landed.at[k], landedu.at[k],
                     land_send.at[k], land_recv.at[k], (s, outer))

    def multiply(left, right):
        return lax.dot_general(left, right, (((0,), (0,)), ((), ())), preferred_element_type=jnp.float32)

    def encode(value, code_at, unit_at):
        top = jnp.maximum(jnp.max(jnp.abs(value), axis=0, keepdims=True), TINY)
        code_at[...] = jnp.round(value * (STEPS / top)).astype(jnp.int32).astype(jnp.int16)
        unit_at[...] = top * (1.0 / STEPS)

    def decode(codes, units):
        return codes.astype(jnp.int32).astype(jnp.float32) * units

    def stage(value, away_from_here, part_at, code_at, unit_at):
        @when(away_from_here)
        def _():
            encode(value, code_at, unit_at)

        @when(jnp.logical_not(away_from_here))
        def _():
            part_at[...] = value

    def relayed_block(j):
        return jnp.where(inside, z + orient * j, 0)

    def gathered(i):
        return both(inside, i == 3 * pieces - 1)

    def relay_product(j, k):
        b = relayed_block(j)
        far_x, far_y = apart(b)
        for side in range(2):
            stage(multiply(got[b, k], rim[:, side * half : (side + 1) * half]), (far_x, far_y)[side],
                  rpart.at[j, k, side], rcode.at[j, k, side], runit.at[j, k, side])

        @when(far_x)
        def _():
            ra1_copy(j, k).start()

        @when(far_y)
        def _():
            rb1_copy(j, k).start()

    def relay_combine(j, k):
        far_x, far_y = apart(relayed_block(j))

        @when(both(jnp.logical_not(far_x), far_y))
        def _():
            ra1_copy(j, k).wait_recv()
            encode(rpart[j, k, 0] + decode(rfrom_x[relayed_block(j) // 2, k], rfrom_xu[relayed_block(j) // 2, k]), rcode.at[j, k, 0], runit.at[j, k, 0])
            ra2_copy(j, k).start()

        @when(both(far_x, jnp.logical_not(far_y)))
        def _():
            rb1_copy(j, k).wait_recv()
            encode(rpart[j, k, 1] + decode(rfrom_y[relayed_block(j) % 2, k], rfrom_yu[relayed_block(j) % 2, k]), rcode.at[j, k, 1], runit.at[j, k, 1])
            rb2_copy(j, k).start()

    def product(i):
        away, k, sign, b, valid, second, relay = place(i)
        far_x, far_y = apart(b)
        passes = onward(away, k, sign, valid)

        @when(valid)
        def _():
            @when(away > 0)
            def _():
                for j in (*chunks(core), *chunks(1 - core)):
                    fwd_copy(b, k, j, sign).wait_recv()

                    @when(passes)
                    def _():
                        fwd_copy(b, k, j, sign).start()

                @when(both(inside, b == outer))
                def _():
                    share_copy(k).start()
                    rim[:, own_columns(k)] = got[b, k]

            @when(both(inside, away == 2, k < relayed))
            def _():
                relay_product(depth - 2, k)

            for side in range(2):
                stage(multiply(got[b, k], feats[:, side * half : (side + 1) * half]), (far_x, far_y)[side],
                      part.at[b, k, side], code.at[b, k, side], unit.at[b, k, side])

            @when(far_x)
            def _():
                a1_copy(b, k).start()

            @when(far_y)
            def _():
                b1_copy(b, k).start()

        @when(gathered(i))
        def _():
            for p in range(pieces):
                share_copy(p).wait_recv()

            lax.fori_loop(0, near * (depth - 2), lambda m, _: (relay_product(m // near, lax.rem(m, near)), 0)[1], 0)

    home = (quad - z) * orient

    def hand_over(k):
        ra1_copy(home, k).wait_recv()
        ra2_copy(home, k).wait_recv()
        encode(rpart[home, k, 0] + decode(rfrom_x[y, k], rfrom_xu[y, k]) + decode(rsum_y[k], rsum_yu[k]),
               ready.at[k, :, 0:half], readyu.at[k, :, 0:half])
        rb1_copy(home, k).wait_recv()
        rb2_copy(home, k).wait_recv()
        encode(rpart[home, k, 1] + decode(rfrom_y[x, k], rfrom_yu[x, k]) + decode(rsum_x[k], rsum_xu[k]),
               ready.at[k, :, half : 2 * half], readyu.at[k, :, half : 2 * half])
        land_copy(k).start()

    def hand_over_early(i):
        @when(both(inside, quad != outer, home < depth - 2, i == base + 2))
        def _():
            lax.fori_loop(0, near, lambda k, _: (hand_over(k), 0)[1], 0)

        for k in range(relayed):
            @when(both(inside, home == depth - 2, i == base + (2, 6, 7)[k]))
            def _():
                hand_over(k)

    def combine(i):
        _, k, _, b, valid, _, relay = place(i)
        far_x, far_y = apart(b)

        @when(both(valid, jnp.logical_not(far_x), far_y))
        def _():
            a1_copy(b, k).wait_recv()
            encode(part[b, k, 0] + decode(from_x[b // 2, k], from_xu[b // 2, k]), code.at[b, k, 0], unit.at[b, k, 0])
            a2_copy(b, k).start()

        @when(both(valid, far_x, jnp.logical_not(far_y)))
        def _():
            b1_copy(b, k).wait_recv()
            encode(part[b, k, 1] + decode(from_y[b % 2, k], from_yu[b % 2, k]), code.at[b, k, 1], unit.at[b, k, 1])
            b2_copy(b, k).start()

        @when(gathered(i))
        def _():
            lax.fori_loop(0, near * (depth - 2), lambda m, _: (relay_combine(m // near, lax.rem(m, near)), 0)[1], 0)

        @when(both(relay, k < relayed))
        def _():
            relay_combine(depth - 2, k)

    base = 3 * pieces

    def sent(k, _):
        for side in range(2):
            pair_copy(side * pieces + k, own_rows).wait_send()

        @when(goes_up(k))
        def _():
            piece_sent(k, up_send.at[k])

        @when(goes_down(k))
        def _():
            piece_sent(k, down_send.at[k])

        @when(inside)
        def _():
            share_copy(k).wait_send()

        return 0

    def sent_late(i, _):
        away, k, sign, b, valid, _, relay = place(i)
        far_x, far_y = apart(b)

        @when(onward(away, k, sign, valid))
        def _():
            piece_sent(k, fwd_send.at[b, k])

        @when(both(valid, far_x))
        def _():
            a1_copy(b, k).wait_send()

        @when(both(valid, far_y))
        def _():
            b1_copy(b, k).wait_send()

        @when(both(valid, jnp.logical_not(far_x), far_y))
        def _():
            a2_copy(b, k).wait_send()

        @when(both(valid, far_x, jnp.logical_not(far_y)))
        def _():
            b2_copy(b, k).wait_send()

        return 0

    def main(i, _):
        @when(both(i >= base, lax.rem(i, 2) == 0))
        def _():
            combine(i - 1)
            combine(i - 2)

        hand_over_early(i)

        @when(both(i >= base, i < steps))
        def _():
            sent_late(i - base, 0)

        @when(both(i >= base, i < base + pieces))
        def _():
            sent(i - base, 0)

        @when(i < steps)
        def _():
            product(i)

        @when(both(i > pieces, i < base, lax.rem(i, 2) == 1))
        def _():
            combine((i - pieces) // 2)

            @when(i > pieces + 1)
            def _():
                combine(i - 3)
                combine(i - 2)

        return 0

    lax.fori_loop(0, steps + 1, main, 0)

    for step in range(1, peers):
        cnt_copy(step, lax.rem(s + peers - step, peers)).wait_recv()
    totals[s] = cnt_ref[...]
    token_total = jnp.sum(totals[...].astype(jnp.float32), axis=0)[0:1, :]
    scale = jnp.broadcast_to(jnp.concatenate([1.0 / token_total] * (half // LANES), axis=1), (LANES, half))

    def local(k):
        return either(inside, k >= quota(jnp.abs(quad - z)), quad == z)

    def finish(k, _):
        at = pl.ds(pl.multiple_of(k * LANES, LANES), LANES)

        @when(local(k))
        def _():
            a1_copy(quad, k).wait_recv()
            a2_copy(quad, k).wait_recv()
            o_ref[at, 0:half] = (part[quad, k, 0] + decode(from_x[y, k], from_xu[y, k])
                                 + decode(sum_y[k], sum_yu[k])) * scale
            b1_copy(quad, k).wait_recv()
            b2_copy(quad, k).wait_recv()
            o_ref[at, half : 2 * half] = (part[quad, k, 1] + decode(from_y[x, k], from_yu[x, k])
                                          + decode(sum_x[k], sum_xu[k])) * scale

        return 0

    lax.fori_loop(0, pieces, finish, 0)

    def take(k, _):
        at = pl.ds(pl.multiple_of(k * LANES, LANES), LANES)

        @when(both(on_rim, quad != z, k < quota(jnp.abs(quad - z))))
        def _():
            land_copy(k).wait_recv()
            for side in range(2):
                cols = slice(side * half, (side + 1) * half)
                o_ref[at, cols] = decode(landed[k, :, cols], landedu[k, :, cols]) * scale

        return 0

    lax.fori_loop(0, relayed, take, 0)

    @when(s < peers - 1)
    def _():
        halo.wait_send()

    for step in range(1, peers):
        cnt_copy(step, s).wait_send()

    lax.fori_loop((steps - base) // 2, steps // 2, lambda n, _: sent_late(2 * n, 0), 0)

    def sent_relayed(m, _):
        j, k = m // relayed, lax.rem(m, relayed)
        far_x, far_y = apart(relayed_block(j))
        live = both(inside, k < quota(j + 1))

        @when(both(live, far_x))
        def _():
            ra1_copy(j, k).wait_send()

        @when(both(live, far_y))
        def _():
            rb1_copy(j, k).wait_send()

        @when(both(live, jnp.logical_not(far_x), far_y))
        def _():
            ra2_copy(j, k).wait_send()

        @when(both(live, far_x, jnp.logical_not(far_y)))
        def _():
            rb2_copy(j, k).wait_send()

        @when(both(live, j == home))
        def _():
            land_copy(k).wait_send()

        return 0

    @when(inside)
    def _():
        lax.fori_loop(0, relayed * (depth - 1), sent_relayed, 0)


def fused_on_device(peers, depth, inputs, conv_weight, conv_bias, doc_start, counts):
    rows, width = inputs.shape
    taps = conv_weight.shape[0]
    half = width // 2
    pieces = half // LANES
    relayed = 3
    vmem = pl.BlockSpec(memory_space=pltpu.VMEM)
    dma = lambda *shape: pltpu.SemaphoreType.DMA(shape)
    f32, i16 = jnp.float32, jnp.int16
    grid = (depth, pieces)
    outs = (depth - 1, relayed)
    return pl.pallas_call(
        functools.partial(gram_kernel, peers, depth, taps, 1, relayed),
        out_shape=jax.ShapeDtypeStruct((half, width), f32),
        in_specs=[pl.BlockSpec(memory_space=pl.ANY)] * 4 + [ pl.BlockSpec(memory_space=pltpu.SMEM)],
        out_specs=vmem,
        scratch_shapes=[
            pltpu.VMEM((rows + HALO, width), inputs.dtype),
            pltpu.VMEM((2 * rows, width), inputs.dtype),
            pltpu.VMEM((depth, pieces, 2 * rows, LANES), inputs.dtype),
            pltpu.VMEM((depth, pieces, 2, LANES, half), f32),
            pltpu.VMEM((2, pieces, LANES, half), i16),
            pltpu.VMEM((2, pieces, LANES, half), i16),
            pltpu.VMEM((pieces, LANES, half), i16),
            pltpu.VMEM((pieces, LANES, half), i16),
            pltpu.VMEM((2 * rows, width), inputs.dtype),
            pltpu.VMEM((*outs, 2, LANES, half), f32),
            pltpu.VMEM((2, relayed, LANES, half), i16),
            pltpu.VMEM((2, relayed, LANES, half), i16),
            pltpu.VMEM((relayed, LANES, half), i16),
            pltpu.VMEM((relayed, LANES, half), i16),
            pltpu.VMEM((relayed, LANES, width), i16),
            pltpu.VMEM((relayed, 1, width), f32),
            pltpu.VMEM((relayed, LANES, width), i16),
            pltpu.VMEM((relayed, 1, width), f32),
            pltpu.VMEM((peers, 8, LANES), jnp.int32),
            pltpu.VMEM((rows, LANES), jnp.int32),
            pltpu.VMEM((8, LANES), jnp.int32),
            pltpu.VMEM((width // LANES, LANES), f32),
            pltpu.VMEM(conv_weight.shape, conv_weight.dtype),
            pltpu.VMEM((width // LANES, LANES), conv_bias.dtype),
            pltpu.VMEM((rows // LANES, LANES), doc_start.dtype),
            dma(3),
            pltpu.VMEM((*grid, 2, LANES, half), i16),
            pltpu.VMEM((*grid, 2, 1, half), f32),
            pltpu.VMEM((2, pieces, 1, half), f32),
            pltpu.VMEM((2, pieces, 1, half), f32),
            pltpu.VMEM((pieces, 1, half), f32),
            pltpu.VMEM((pieces, 1, half), f32),
            pltpu.VMEM((*outs, 2, LANES, half), i16),
            pltpu.VMEM((*outs, 2, 1, half), f32),
            pltpu.VMEM((2, relayed, 1, half), f32),
            pltpu.VMEM((2, relayed, 1, half), f32),
            pltpu.VMEM((relayed, 1, half), f32),
            pltpu.VMEM((relayed, 1, half), f32),
            pltpu.SemaphoreType.DMA, dma(2), dma(peers), dma(peers), dma(2 * pieces), dma(2 * pieces),
            dma(pieces), dma(pieces), dma(*grid), dma(*grid, 4),
            dma(2, pieces, 2), dma(2, pieces, 2), dma(2, pieces, 2), dma(2, pieces, 2),
            dma(pieces, 2), dma(pieces, 2), dma(pieces, 2), dma(pieces, 2),
            dma(pieces), dma(pieces),
            dma(2, relayed, 2), dma(2, relayed, 2), dma(2, relayed, 2), dma(2, relayed, 2),
            dma(relayed, 2), dma(relayed, 2), dma(relayed, 2), dma(relayed, 2), dma(relayed, 2), dma(relayed, 2),
        ],
        compiler_params=pltpu.CompilerParams(collective_id=0, has_side_effects=True,
                                             vmem_limit_bytes=52480 * 1024),
        name="gram",
    )(inputs, *(pltpu.with_memory_space_constraint(a, pltpu.HBM) for a in (conv_weight, conv_bias.reshape(width // LANES, LANES), doc_start.reshape(rows // LANES, LANES))), counts)


def passed_along(x, axis, by):
    peers = lax.axis_size(axis)
    pairs = [(i, i + by) for i in range(peers) if 0 <= i + by < peers]
    return lax.ppermute(x, axis, pairs)


def causal_conv(extended, weights, bias, position, doc_start, length):
    kernel_len = weights.shape[0]
    summed = jnp.zeros((length, weights.shape[1]), jnp.float32) + bias.astype(jnp.float32)
    for lag in range(kernel_len):
        window = extended[kernel_len - 1 - lag : kernel_len - 1 - lag + length].astype(jnp.float32)
        usable = position - lag >= doc_start
        summed = summed + jnp.where(usable[:, None], weights[lag].astype(jnp.float32) * window, 0.0)
    return jax.nn.silu(summed).astype(jnp.bfloat16)


def on_device(inputs, conv_weight, conv_bias, doc_start, counts):
    row_count = inputs.shape[0]
    kernel_len = conv_weight.shape[0]
    position = lax.axis_index("seq") * row_count + jnp.arange(row_count, dtype=jnp.int32)
    counted = jnp.arange(row_count, dtype=jnp.int32) < counts[0]
    token_total = lax.psum(counts.astype(jnp.float32)[0], "seq")
    prior = passed_along(inputs[row_count - (kernel_len - 1) :], "seq", 1)
    extended = jnp.concatenate([prior, inputs], axis=0)
    own_feats = causal_conv(extended, conv_weight, conv_bias, position, doc_start, row_count)
    kept = jnp.where(counted[:, None], own_feats, jnp.zeros_like(own_feats))
    whole = lax.all_gather(own_feats, "mp", axis=1, tiled=True)
    summed = lax.psum_scatter(
        lax.dot_general(whole, kept, (((0,), (0,)), ((), ())), preferred_element_type=jnp.float32),
        "seq",
        scatter_dimension=0,
        tiled=True,
    )
    return summed / token_total


def solution(mesh):
    placed = (P("seq", "mp"), P(None, "mp"), P("mp"), P("seq"), P("seq"))
    peers, depth = mesh.shape["seq"], mesh.shape["mp"]
    fits = peers == 2 * depth and depth == 2**2
    body = functools.partial(fused_on_device, peers, depth) if fits else on_device
    return jax.shard_map(body, mesh=mesh, in_specs=placed, out_specs=P("seq", "mp"), check_vma=False)
```
